128 devices in a mesh: dp: 128 (over z, y, x, core).
Axes of the slice: x: 4, y: 4, z: 4, core: 2. Of those that a mesh axis runs over, the one named last changes fastest.
Arguments:
- grads: float32 [128, 4194304], P('dp')
- master: float32 [4194304], P('dp'), may hold values from -0.75 to 0.75
- m_old: float32 [128, 65536], P('dp'), may hold values from -6 to 6
- v_old: float32 [128, 65536], P('dp'), may hold values from 0.25 to 4
- old_bounds: int32 [129], replicated, may hold values from 0 to 4194304, as said below
Outputs:
- master_new: float32 [4194304], P('dp')
- m_new: float32 [4194304], P('dp')
- v_new: float32 [4194304], P('dp')
- params_full: bfloat16 [4194304], replicated
The draws below stay inside these ranges and needn't reach their ends.
Inputs may be any that keep to these rules, and one draw needn't show every extreme that they name: old_bounds[0] = 0, the last entry is 4194304, entries never fall, and old_bounds[i] - i * 32768 lies between -16384 and 16384 for every i. Row k of m_old and v_old holds its span in its first old_bounds[k+1] - old_bounds[k] slots; later slots are unused. Some span has exactly 65536 entries in every draw.
All inputs are finite; a program needn't handle non-finite values.
Results may differ from the reference program's by a relative error of at most 0.0049.
Values may be sent and summed in bfloat16 or wider, within the bound.
No kernel may reach another device: no remote copies, remote signals or barrier semaphores. Data moves between devices by JAX's collectives and lax.ppermute only.
A program may use at most 128 MiB of HBM per device.

```python
import math
import jax
import jax.numpy as jnp
from jax import lax

ND = 32768
FLAT = 4194304
CAP = 65536
N_DP = 128


def draw_grads(key, part):
    first = jax.random.fold_in(jax.random.fold_in(key, 21), 0)
    fourth = jax.random.fold_in(jax.random.fold_in(key, 21), 3)
    fifth = jax.random.fold_in(jax.random.fold_in(key, 21), 4)
    positions = jnp.arange(FLAT, dtype=jnp.float32)
    ramp = 1.0 + 2.0 * positions / FLAT
    block_level = jnp.exp(jax.random.uniform(fourth, (N_DP, 1), jnp.float32, -0.8, 0.8))
    level = (block_level * jnp.ones((1, ND), jnp.float32)).reshape(FLAT)
    overall = jnp.exp(jax.random.uniform(fifth, (), jnp.float32, -1.0, 1.0))
    values = jax.random.normal(first, (N_DP, FLAT), jnp.float32) * (ramp * level * overall)
    return values.astype(jnp.float32)


def draw_old_bounds(key, part):
    first, second = jax.random.split(jax.random.fold_in(key, 11))
    margin = ND // 2
    drift = jax.random.randint(first, (N_DP + 1,), -margin, margin + 1)
    chosen = jax.random.randint(second, (), 1, N_DP - 1)
    index_all = jnp.arange(N_DP + 1, dtype=jnp.int32)
    drift = jnp.where(index_all == chosen, -margin, drift)
    drift = jnp.where(index_all == chosen + 1, margin, drift)
    drift = jnp.where((index_all == 0) | (index_all == N_DP), 0, drift)
    return (index_all * ND + drift).astype(jnp.int32)


def block_scale(stream_key, extent, cuts, low, largest):
    loudness, own = 1.0, jax.random.fold_in(stream_key, 6)
    for position, shards_of in cuts:
        heights = jnp.exp(jax.random.uniform(jax.random.fold_in(own, position), (shards_of,), jnp.float32, low / len(cuts), largest / len(cuts)))
        loudness = loudness * jnp.repeat(heights, extent[position] // shards_of).reshape([-1 if axis == position else 1 for axis in range(len(extent))])
    return loudness


def centred(stream_key, dims, deviation, bound, shards=(), kind=jnp.bfloat16):
    drawn = jax.random.normal(stream_key, dims, jnp.float32) * deviation
    if len(shards) > 0:
        drawn = block_scale(stream_key, dims, shards, -0.22, 0.18) * drawn
    return jnp.clip(drawn, min=-bound, max=bound).astype(kind)


def setup_inputs(seed: int = 0) -> dict:
    key_list = jax.random.split(jax.random.key(seed), 6)
    return {
        "grads": draw_grads(jax.random.fold_in(key_list[5], 71), 0),
        "master": centred(key_list[1], (FLAT,), 0.05, 0.75, ((0, 128),), jnp.float32),
        "m_old": centred(key_list[2], (N_DP, CAP), 1.0, 6.0, ((0, 128),), jnp.float32),
        "v_old": jnp.clip(jnp.exp(math.log(4.0) - 2.7725887 * jax.random.uniform(key_list[3], (N_DP, CAP), jnp.float32) ** block_scale(key_list[3], (N_DP, CAP), ((0, 128),), -0.2, 0.2)), 0.25, 4.0),
        "old_bounds": draw_old_bounds(jax.random.fold_in(key_list[5], 71), 0),
    }


def reference(grads, master, m_old, v_old, old_bounds):
    gradient = lax.optimization_barrier(jnp.sum(grads, axis=0))
    positions = jnp.arange(FLAT, dtype=jnp.int32)
    owner = (jnp.searchsorted(old_bounds, positions, side='right') - 1).astype(jnp.int32)
    slot = (positions - old_bounds[owner]).astype(jnp.int32)
    m_prev = m_old[owner, slot]
    v_prev = v_old[owner, slot]
    total = jnp.sum(gradient * gradient)
    clip = jnp.minimum(1.0, jnp.sqrt(jnp.float32(FLAT)) / (jnp.sqrt(total) + 1e-06))
    clipped = clip * gradient
    m_new = 0.5 * m_prev + 0.5 * clipped
    v_new = 0.95 * v_prev + 0.05 * clipped * clipped
    direction = m_new / (1.0 - 0.5 ** 20) / (jnp.sqrt(v_new / (1.0 - 0.95 ** 20)) + 1e-08)
    master_new = master - 0.05 * (direction + 0.1 * master)
    return (master_new, m_new, v_new, master_new.astype(jnp.bfloat16))
```

```python
import jax
import jax.numpy as jnp
from jax import lax
from jax.experimental import pallas as pl
from jax.experimental.pallas import tpu as pltpu
from jax.sharding import Mesh
from jax.sharding import PartitionSpec as P

DP = ("z", "y", "x", "core")
BF = jnp.bfloat16
F32 = jnp.float32


def coords(d):
    return d // 32, d // 8 % 4, d // 2 % 4, d % 2


def shard_of(z, y, x, c):
    return ((z * 4 + y) * 4 + x) * 2 + c


def perm(axis, s):
    pairs = []
    for d in range(128):
        z, y, x, c = coords(d)
        if axis == "core":
            c = 1 - c
        elif axis == "z":
            z = (z + s) % 4
        elif (axis == "a") == (c == 0):
            x = (x + s) % 4
        else:
            y = (y + s) % 4
        pairs.append((d, shard_of(z, y, x, c)))
    return pairs


def send(value, axis, s=1):
    return lax.ppermute(value, DP, perm(axis, s))


def table(c, z, y, x, s):
    i = jnp.arange(16, dtype=jnp.int32)
    rb, rz = i // 4, i % 4
    zz = (z + rz) % 4
    on_0 = shard_of(zz, (y + rb) % 4, (x + s) % 4, 0)
    on_1 = shard_of(zz, (y + s) % 4, (x + rb) % 4, 1)
    return jnp.where(c == 0, on_0, on_1).astype(jnp.int32)


def picked(rows, lanes):
    return [
        pl.BlockSpec((1, rows, lanes), lambda i, t, j=j: (t[4 * i + j], 0, 0)) for j in range(4)
    ]


def cost(flops, nbytes):
    return pl.CostEstimate(flops=flops, transcendentals=0, bytes_accessed=nbytes)


def convert_piece(t, g):
    _, rows, lanes = g.shape

    def body(t_ref, g0, g1, g2, g3, o):
        for j, r in enumerate((g0, g1, g2, g3)):
            o[j] = r[0].astype(BF)

    block = pl.BlockSpec((4, rows, lanes), lambda i, t: (i, 0, 0))
    n = 16 * rows * lanes
    return pl.pallas_call(
        body,
        grid_spec=pltpu.PrefetchScalarGridSpec(
            num_scalar_prefetch=1, grid=(4,), in_specs=picked(rows, lanes), out_specs=block
        ),
        out_shape=jax.ShapeDtypeStruct((16, rows, lanes), BF),
        cost_estimate=cost(n, 6 * n),
    )(t, g, g, g, g)


def sum_piece(t, g, other):
    _, rows, lanes = g.shape

    def body(t_ref, g0, g1, g2, g3, r, o):
        for j, v in enumerate((g0, g1, g2, g3)):
            o[j] = (v[0] + r[j].astype(F32)).astype(BF)

    block = pl.BlockSpec((4, rows, lanes), lambda i, t: (i, 0, 0))
    n = 16 * rows * lanes
    return pl.pallas_call(
        body,
        grid_spec=pltpu.PrefetchScalarGridSpec(
            num_scalar_prefetch=1, grid=(4,), in_specs=picked(rows, lanes) + [block], out_specs=block
        ),
        out_shape=jax.ShapeDtypeStruct((16, rows, lanes), BF),
        cost_estimate=cost(n, 8 * n),
    )(t, g, g, g, g, other)


def sum_own(t, g, other, r1, r2, r3):
    _, rows, lanes = g.shape

    def body(t_ref, g0, g1, g2, g3, ro, ra, rb, rc, own, q1, q2, q3):
        i = pl.program_id(0)

        def value(j, v):
            return (v[0] + ro[j].astype(F32)) + (ra[j].astype(F32) + rc[j].astype(F32)) + rb[j].astype(F32)

        for k, o in enumerate((own, q1, q2, q3)):

            @pl.when(i == k)
            def _(o=o):
                for j, v in enumerate((g0, g1, g2, g3)):
                    o[j] = value(j, v).astype(o.dtype)

    block = pl.BlockSpec((4, rows, lanes), lambda i, t: (i, 0, 0))
    whole = pl.BlockSpec((4, rows, lanes), lambda i, t: (0, 0, 0))
    n = 16 * rows * lanes
    return pl.pallas_call(
        body,
        grid_spec=pltpu.PrefetchScalarGridSpec(
            num_scalar_prefetch=1,
            grid=(4,),
            in_specs=picked(rows, lanes) + [block] * 4,
            out_specs=[whole] * 4,
        ),
        out_shape=[jax.ShapeDtypeStruct((4, rows, lanes), F32)]
        + [jax.ShapeDtypeStruct((4, rows, lanes), BF)] * 3,
        cost_estimate=cost(4 * n, 14 * n),
    )(t, g, g, g, g, other, r1, r2, r3)


def place(t, piece, out):
    n, rows, lanes = piece.shape

    def body(t_ref, p, *refs):
        o, sem = refs[-2], refs[-1]
        copies = [pltpu.make_async_copy(p.at[i], o.at[t_ref[i]], sem.at[i]) for i in range(n)]
        for copy in copies:
            copy.start()
        for copy in copies:
            copy.wait()

    anywhere = pl.BlockSpec(memory_space=pl.ANY)
    operands = [t, piece] + ([] if out is None else [out])
    return pl.pallas_call(
        body,
        grid_spec=pltpu.PrefetchScalarGridSpec(
            num_scalar_prefetch=1,
            grid=(1,),
            in_specs=[anywhere] * (len(operands) - 1),
            out_specs=anywhere,
            scratch_shapes=[pltpu.SemaphoreType.DMA((n,))],
        ),
        out_shape=jax.ShapeDtypeStruct((128, rows, lanes), BF),
        input_output_aliases={} if out is None else {2: 0},
        cost_estimate=cost(n * rows * lanes, 4 * n * rows * lanes),
    )(*operands)


def shifted(value, steps):
    leading, last = (max(0, -steps), min(128, 128 - steps))
    return lax.ppermute(value, DP, [(source, source + steps) for source in range(leading, last)])


def window(buffer, offset, width):
    padded = jnp.pad(buffer, ((0, 0), (2 * width, width)))
    return lax.dynamic_slice_in_dim(padded, offset + 2 * width, width, 1)


def old_moments(m_old, v_old, old_bounds, device, width):
    packed = jnp.stack([m_old[0], v_old[0]])
    from_before = shifted(packed.astype(BF), 1).astype(packed.dtype)
    from_after = shifted(packed.astype(BF), -1).astype(packed.dtype)
    start = device * width
    bound_before = old_bounds[jnp.maximum(device - 1, 0)]
    bound_here = old_bounds[device]
    bound_after = old_bounds[device + 1]
    part_before = window(from_before, start - bound_before, width)
    part_here = window(packed, start - bound_here, width)
    part_after = window(from_after, start - bound_after, width)
    positions = start + jnp.arange(width, dtype=jnp.int32)
    moments = jnp.where(
        positions[None, :] < bound_here,
        part_before,
        jnp.where(positions[None, :] >= bound_after, part_after, part_here),
    )
    return moments[0], moments[1]


def local(grads, master, m_old, v_old, old_bounds):
    count = 128
    width = master.shape[0]
    rows = width // 128
    device = lax.axis_index(DP)
    z, y, x, c = coords(device)
    mine = [table(c, z, y, x, s) for s in range(4)]
    theirs = [table(1 - c, z, y, x, s) for s in range(4)]
    g = grads[0].reshape(128, rows, 128)

    swapped = {}
    for s in (2, 1, 3, 0):
        swapped[s] = send(convert_piece(theirs[s], g), "core")
    ringed = {}
    for s in (2, 1, 3):
        ringed[s] = send(sum_piece(mine[s], g, swapped[s]), "a", s)
    m_prev, v_prev = old_moments(m_old, v_old, old_bounds, device, width)
    own, q1, q2, q3 = sum_own(mine[0], g, swapped[0], ringed[1], ringed[2], ringed[3])
    q2, q1, q3 = send(q2, "b", 2), send(q1, "b", 1), send(q3, "b", 3)
    partial = own + (q1.astype(F32) + q3.astype(F32)) + q2.astype(F32)
    w = [partial[s].astype(BF) for s in range(4)]
    w2, w1, w3 = send(w[2], "z", 2), send(w[1], "z", 1), send(w[3], "z", 3)
    gradient = partial[0] + (w1.astype(F32) + w3.astype(F32)) + w2.astype(F32)

    squares = jnp.sum(gradient * gradient)
    total = jnp.sum(lax.all_to_all(jnp.broadcast_to(squares, (count,)), DP, 0, 0, tiled=True))
    clip = jnp.minimum(1.0, jnp.sqrt(jnp.float32(count * width)) / (jnp.sqrt(total) + 1e-06))
    clipped = clip * gradient.reshape(width)
    m_new = 0.5 * m_prev + 0.5 * clipped
    v_new = 0.95 * v_prev + 0.05 * clipped * clipped
    direction = m_new / (1.0 - 0.5**20) / (jnp.sqrt(v_new / (1.0 - 0.95**20)) + 1e-08)
    master_new = master - 0.05 * (direction + 0.1 * master)

    piece = master_new.astype(BF).reshape(1, rows, 128)
    for axis in ("z", "b"):
        got = {s: send(piece, axis, s) for s in (2, 1, 3)}
        piece = jnp.concatenate([piece, got[3], got[2], got[1]])
    got = {0: piece}
    for s in (2, 1, 3):
        got[(4 - s) % 4] = send(piece, "a", s)
    out = None
    for s in (0, 2, 3, 1):
        other = send(got[s], "core")
        out = place(mine[s], got[s], out)
        out = place(theirs[s], other, out)
    return (master_new, m_new, v_new, out.reshape(count * width))


def solution(mesh):
    finer = Mesh(mesh.devices.reshape(4, 4, 4, 2), DP)
    placed = (P(DP, None), P(DP), P(DP, None), P(DP, None), P())
    return jax.shard_map(
        local, mesh=finer, in_specs=placed, out_specs=(P(DP), P(DP), P(DP), P()), check_vma=False
    )
```

```python
import jax
import jax.numpy as jnp
from jax import lax
from jax.experimental import pallas as pl
from jax.experimental.pallas import tpu as pltpu
from jax.sharding import Mesh
from jax.sharding import PartitionSpec as P

DP = ("z", "y", "x", "core")
BF = jnp.bfloat16
F32 = jnp.float32


def coords(d):
    return d // 32, d // 8 % 4, d // 2 % 4, d % 2


def shard_of(z, y, x, c):
    return ((z * 4 + y) * 4 + x) * 2 + c


def perm(axis, s):
    pairs = []
    for d in range(128):
        z, y, x, c = coords(d)
        if axis == "core":
            c = 1 - c
        elif axis == "z":
            z = (z + s) % 4
        elif (axis == "a") == (c == 0):
            x = (x + s) % 4
        else:
            y = (y + s) % 4
        pairs.append((d, shard_of(z, y, x, c)))
    return pairs


def send(value, axis, s=1):
    return lax.ppermute(value, DP, perm(axis, s))


def table(c, z, y, x, s):
    i = jnp.arange(16, dtype=jnp.int32)
    rb, rz = i // 4, i % 4
    zz = (z + rz) % 4
    on_0 = shard_of(zz, (y + rb) % 4, (x + s) % 4, 0)
    on_1 = shard_of(zz, (y + s) % 4, (x + rb) % 4, 1)
    return jnp.where(c == 0, on_0, on_1).astype(jnp.int32)


def cost(flops, nbytes):
    return pl.CostEstimate(flops=flops, transcendentals=0, bytes_accessed=nbytes)


def gathered_call(body, t, operands, outs, scratch, flops, nbytes):
    anywhere = pl.BlockSpec(memory_space=pl.ANY)
    return pl.pallas_call(
        body,
        grid_spec=pltpu.PrefetchScalarGridSpec(
            num_scalar_prefetch=1,
            grid=(1,),
            in_specs=[anywhere] * len(operands),
            out_specs=[anywhere] * len(outs),
            scratch_shapes=scratch,
        ),
        out_shape=outs,
        cost_estimate=cost(flops, nbytes),
    )(t, *operands)


def sum_piece(t, g, others=(), split=False):
    _, rows, lanes = g.shape
    m = len(others)

    def body(t_ref, g_ref, *refs):
        ins, rest = refs[:m], refs[m:]
        n_out = 4 if split else 1
        outs, rest = rest[:n_out], rest[n_out:]
        g_buf, rest = rest[0], rest[1:]
        bufs, rest = rest[:m], rest[m:]
        stages, (in_sem, out_sem) = rest[:-2], rest[-2:]

        def reads(i):
            yield pltpu.make_async_copy(g_ref.at[t_ref[i]], g_buf.at[i], in_sem.at[0, i])
            for k in range(m):
                yield pltpu.make_async_copy(ins[k].at[i], bufs[k].at[i], in_sem.at[k + 1, i])

        for i in range(16):
            for copy in reads(i):
                copy.start()
        writes = []
        for i in range(16):
            for copy in reads(i):
                copy.wait()
            value = g_buf[i]
            for k in range(m):
                value = value + bufs[k][i].astype(F32)
            q, at = (i // 4, i % 4) if split else (0, i)
            stages[q][at] = value.astype(stages[q].dtype)
            writes.append(pltpu.make_async_copy(stages[q].at[at], outs[q].at[at], out_sem.at[i]))
            writes[-1].start()
        for copy in writes:
            copy.wait()

    if split:
        types = [((4, rows, lanes), F32)] + [((4, rows, lanes), BF)] * 3
    else:
        types = [((16, rows, lanes), BF)]
    scratch = [pltpu.VMEM((16, rows, lanes), F32)] + [pltpu.VMEM((16, rows, lanes), BF)] * m
    scratch += [pltpu.VMEM(*kind) for kind in types]
    scratch += [pltpu.SemaphoreType.DMA((m + 1, 16)), pltpu.SemaphoreType.DMA((16,))]
    n = 16 * rows * lanes
    got = gathered_call(
        body, t, (g, *others), [jax.ShapeDtypeStruct(*kind) for kind in types], scratch, (m + 1) * n, (6 + 2 * m) * n
    )
    return got if split else got[0]


def place(t, piece, out):
    n, rows, lanes = piece.shape

    def body(t_ref, p, *refs):
        o, buf, in_sem, out_sem = refs[-4:]
        reads = [pltpu.make_async_copy(p.at[i], buf.at[i], in_sem.at[i]) for i in range(n)]
        writes = [pltpu.make_async_copy(buf.at[i], o.at[t_ref[i]], out_sem.at[i]) for i in range(n)]
        for copy in reads:
            copy.start()
        for i in range(n):
            reads[i].wait()
            writes[i].start()
        for copy in writes:
            copy.wait()

    anywhere = pl.BlockSpec(memory_space=pl.ANY)
    operands = [t, piece] + ([] if out is None else [out])
    return pl.pallas_call(
        body,
        grid_spec=pltpu.PrefetchScalarGridSpec(
            num_scalar_prefetch=1,
            grid=(1,),
            in_specs=[anywhere] * (len(operands) - 1),
            out_specs=anywhere,
            scratch_shapes=[
                pltpu.VMEM((n, rows, lanes), BF),
                pltpu.SemaphoreType.DMA((n,)),
                pltpu.SemaphoreType.DMA((n,)),
            ],
        ),
        out_shape=jax.ShapeDtypeStruct((128, rows, lanes), BF),
        input_output_aliases={} if out is None else {2: 0},
        cost_estimate=cost(n * rows * lanes, 4 * n * rows * lanes),
    )(*operands)


def shifted(value, steps):
    leading, last = (max(0, -steps), min(128, 128 - steps))
    return lax.ppermute(value, DP, [(source, source + steps) for source in range(leading, last)])


def window(buffer, offset, width):
    padded = jnp.pad(buffer, ((0, 0), (2 * width, width)))
    return lax.dynamic_slice_in_dim(padded, offset + 2 * width, width, 1)


def old_moments(m_old, v_old, old_bounds, device, width, after):
    packed = jnp.stack([m_old[0], v_old[0]])
    sent, _ = lax.optimization_barrier((packed.astype(BF), after))
    from_before = shifted(sent, 1).astype(packed.dtype)
    from_after = shifted(sent, -1).astype(packed.dtype)
    start = device * width
    bound_before = old_bounds[jnp.maximum(device - 1, 0)]
    bound_here = old_bounds[device]
    bound_after = old_bounds[device + 1]
    part_before = window(from_before, start - bound_before, width)
    part_here = window(packed, start - bound_here, width)
    part_after = window(from_after, start - bound_after, width)
    positions = start + jnp.arange(width, dtype=jnp.int32)
    moments = jnp.where(
        positions[None, :] < bound_here,
        part_before,
        jnp.where(positions[None, :] >= bound_after, part_after, part_here),
    )
    return moments[0], moments[1]


def local(grads, master, m_old, v_old, old_bounds):
    count = 128
    width = master.shape[0]
    rows = width // 128
    device = lax.axis_index(DP)
    z, y, x, c = coords(device)
    mine = [table(c, z, y, x, s) for s in range(4)]
    theirs = [table(1 - c, z, y, x, s) for s in range(4)]
    g = grads[0].reshape(128, rows, 128)

    swapped = {}
    for s in (2, 1, 3, 0):
        swapped[s] = send(sum_piece(theirs[s], g), "core")
    ringed = {}
    for s in (2, 1, 3):
        piece = sum_piece(mine[s], g, (swapped[s],))
        ringed[s] = send(piece, "a", s)
    m_prev, v_prev = old_moments(m_old, v_old, old_bounds, device, width, piece)
    own, q1, q2, q3 = sum_piece(mine[0], g, (swapped[0], ringed[1], ringed[2], ringed[3]), split=True)
    q2, q1, q3 = send(q2, "b", 2), send(q1, "b", 1), send(q3, "b", 3)
    partial = own + (q1.astype(F32) + q3.astype(F32)) + q2.astype(F32)
    w = [partial[s].astype(BF) for s in range(4)]
    w2, w1, w3 = send(w[2], "z", 2), send(w[1], "z", 1), send(w[3], "z", 3)
    gradient = partial[0] + (w1.astype(F32) + w3.astype(F32)) + w2.astype(F32)

    squares = jnp.sum(gradient * gradient)
    total = jnp.sum(lax.all_to_all(jnp.broadcast_to(squares, (count,)), DP, 0, 0, tiled=True))
    clip = jnp.minimum(1.0, jnp.sqrt(jnp.float32(count * width)) / (jnp.sqrt(total) + 1e-06))
    clipped = clip * gradient.reshape(width)
    m_new = 0.5 * m_prev + 0.5 * clipped
    v_new = 0.95 * v_prev + 0.05 * clipped * clipped
    direction = m_new / (1.0 - 0.5**20) / (jnp.sqrt(v_new / (1.0 - 0.95**20)) + 1e-08)
    master_new = master - 0.05 * (direction + 0.1 * master)

    piece = master_new.astype(BF).reshape(1, rows, 128)
    for axis in ("z", "b"):
        got = {s: send(piece, axis, s) for s in (2, 1, 3)}
        piece = jnp.concatenate([piece, got[3], got[2], got[1]])
    got = {0: piece}
    for s in (2, 1, 3):
        got[(4 - s) % 4] = send(piece, "a", s)
    out = None
    for s in (0, 2, 3, 1):
        other = send(got[s], "core")
        out = place(mine[s], got[s], out)
        out = place(theirs[s], other, out)
    return (master_new, m_new, v_new, out.reshape(count * width))


def solution(mesh):
    finer = Mesh(mesh.devices.reshape(4, 4, 4, 2), DP)
    placed = (P(DP, None), P(DP), P(DP, None), P(DP, None), P())
    return jax.shard_map(
        local, mesh=finer, in_specs=placed, out_specs=(P(DP), P(DP), P(DP), P()), check_vma=False
    )
```

```python
import jax
import jax.numpy as jnp
from jax import lax
from jax.experimental import pallas as pl
from jax.experimental.pallas import tpu as pltpu
from jax.sharding import Mesh
from jax.sharding import PartitionSpec as P

DP = ("z", "y", "x", "core")
BF = jnp.bfloat16
F32 = jnp.float32


def coords(d):
    return d // 32, d // 8 % 4, d // 2 % 4, d % 2


def shard_of(z, y, x, c):
    return ((z * 4 + y) * 4 + x) * 2 + c


def perm(axis, s):
    pairs = []
    for d in range(128):
        z, y, x, c = coords(d)
        if axis == "core":
            c = 1 - c
        elif axis == "z":
            z = (z + s) % 4
        elif (axis == "a") == (c == 0):
            x = (x + s) % 4
        else:
            y = (y + s) % 4
        pairs.append((d, shard_of(z, y, x, c)))
    return pairs


def send(value, axis, s=1):
    return lax.ppermute(value, DP, perm(axis, s))


def table(c, z, y, x, s):
    i = jnp.arange(16, dtype=jnp.int32)
    rb, rz = i // 4, i % 4
    zz = (z + rz) % 4
    on_0 = shard_of(zz, (y + rb) % 4, (x + s) % 4, 0)
    on_1 = shard_of(zz, (y + s) % 4, (x + rb) % 4, 1)
    return jnp.where(c == 0, on_0, on_1).astype(jnp.int32)


def cost(flops, nbytes):
    return pl.CostEstimate(flops=flops, transcendentals=0, bytes_accessed=nbytes)


def call(body, t, operands, outs, scratch, flops, nbytes, aliases=None, spaces=None, limit=2):
    vmem = pl.BlockSpec(memory_space=pltpu.VMEM)
    hbm = pl.BlockSpec(memory_space=pltpu.HBM)
    spaces = spaces or [True] * len(operands)
    operands = [pltpu.with_memory_space_constraint(o, pltpu.VMEM if v else pltpu.HBM) for o, v in zip(operands, spaces)]
    return pl.pallas_call(
        body,
        grid_spec=pltpu.PrefetchScalarGridSpec(
            num_scalar_prefetch=1,
            grid=(1,),
            in_specs=[vmem if v else hbm for v in spaces],
            out_specs=[hbm if isinstance(o, jax.ShapeDtypeStruct) else vmem for o in outs],
            scratch_shapes=scratch,
        ),
        out_shape=outs,
        input_output_aliases=aliases or {},
        cost_estimate=cost(flops, nbytes),
        compiler_params=pltpu.CompilerParams(vmem_limit_bytes=limit * 2**20),
    )(t, *operands)


def fetch(t, g, dtype):
    _, rows, lanes = g.shape
    whole = dtype == g.dtype

    def body(t_ref, g_ref, *refs):
        outs, (*buf, sem) = refs[:4], refs[4:]
        to = [outs[i // 16].at[i % 16] if whole else buf[0].at[i] for i in range(64)]
        copies = [pltpu.make_async_copy(g_ref.at[t_ref[i]], to[i], sem.at[i]) for i in range(64)]
        for copy in copies:
            copy.start()
        for i, copy in enumerate(copies):
            copy.wait()
            if not whole:
                outs[i // 16][i % 16] = buf[0][i].astype(dtype)

    scratch = [] if whole else [pltpu.VMEM((64, rows, lanes), g.dtype)]
    n = 64 * rows * lanes
    return call(
        body,
        t,
        (g,),
        [pltpu.VMEM((16, rows, lanes), dtype)] * 4,
        scratch + [pltpu.SemaphoreType.DMA((64,))],
        n,
        6 * n,
        spaces=[False],
        limit=12,
    )


def sum_piece(parts, split=False):
    n, rows, lanes = parts[0].shape
    m = len(parts)

    def body(t_ref, *refs):
        ins, outs = refs[:m], refs[m:]
        each = n // len(outs)

        for q, o in enumerate(outs):

            @pl.loop(0, each)
            def _(i, q=q, o=o):
                value = ins[0][q * each + i].astype(F32)
                for r in ins[1:]:
                    value = value + r[q * each + i].astype(F32)
                o[i] = value.astype(o.dtype)

    if split:
        outs = [pltpu.VMEM((4, rows, lanes), F32)] + [pltpu.VMEM((4, rows, lanes), BF)] * 3
    else:
        outs = [pltpu.VMEM((16, rows, lanes), BF)]
    size = n * rows * lanes
    got = call(body, jnp.zeros((1,), jnp.int32), parts, outs, [], m * size, (6 + 2 * m) * size)
    return got if split else got[0]


def place(pairs, out):
    k = len(pairs)
    n, rows, lanes = pairs[0][1].shape

    def body(t_ref, *refs):
        o, sem = refs[-2:]
        copies = [
            pltpu.make_async_copy(refs[j].at[i], o.at[t_ref[j * n + i]], sem.at[j * n + i])
            for j in range(k)
            for i in range(n)
        ]
        for copy in copies:
            copy.start()
        for copy in copies:
            copy.wait()

    t = jnp.concatenate([p[0] for p in pairs])
    operands = [p[1] for p in pairs] + ([] if out is None else [out])
    nbytes = 4 * k * n * rows * lanes
    return call(
        body,
        t,
        operands,
        [jax.ShapeDtypeStruct((128, rows, lanes), BF)],
        [pltpu.SemaphoreType.DMA((k * n,))],
        nbytes,
        nbytes,
        {} if out is None else {k + 1: 0},
        [True] * k + [False] * (0 if out is None else 1),
    )[0]


def shifted(value, steps):
    leading, last = (max(0, -steps), min(128, 128 - steps))
    return lax.ppermute(value, DP, [(source, source + steps) for source in range(leading, last)])


def window(buffer, offset, width):
    padded = jnp.pad(buffer, ((0, 0), (2 * width, width)))
    return lax.dynamic_slice_in_dim(padded, offset + 2 * width, width, 1)


def old_moments(m_old, v_old, old_bounds, device, width, after):
    packed = jnp.stack([m_old[0], v_old[0]])
    sent, _ = lax.optimization_barrier((packed.astype(BF), after))
    from_before = shifted(sent, 1).astype(packed.dtype)
    from_after = shifted(sent, -1).astype(packed.dtype)
    start = device * width
    bound_before = old_bounds[jnp.maximum(device - 1, 0)]
    bound_here = old_bounds[device]
    bound_after = old_bounds[device + 1]
    part_before = window(from_before, start - bound_before, width)
    part_here = window(packed, start - bound_here, width)
    part_after = window(from_after, start - bound_after, width)
    positions = start + jnp.arange(width, dtype=jnp.int32)
    moments = jnp.where(
        positions[None, :] < bound_here,
        part_before,
        jnp.where(positions[None, :] >= bound_after, part_after, part_here),
    )
    return moments[0], moments[1]


def step(grads, master, m_old, v_old, old_bounds):
    count = 128
    width = master.shape[0]
    rows = width // 128
    device = lax.axis_index(DP)
    z, y, x, c = coords(device)
    mine = [table(c, z, y, x, s) for s in range(4)]
    theirs = [table(1 - c, z, y, x, s) for s in range(4)]
    g = grads[0].reshape(128, rows, 128)

    order = (2, 1, 3, 0)
    given = fetch(jnp.concatenate([theirs[s] for s in order]), g, BF)
    swapped = {s: send(v, "core") for s, v in zip(order, given)}
    kept = fetch(jnp.concatenate([mine[s] for s in order]), g, F32)
    kept = dict(zip(order, kept))
    ringed = {}
    for s in (2, 1, 3):
        piece = sum_piece((kept[s], swapped[s]))
        ringed[s] = send(piece, "a", s)
    m_prev, v_prev = old_moments(m_old, v_old, old_bounds, device, width, piece)
    ringed[3], m_prev, v_prev = lax.optimization_barrier((ringed[3], m_prev, v_prev))
    own, q1, q2, q3 = sum_piece((kept[0], swapped[0], ringed[1], ringed[2], ringed[3]), split=True)
    q2, q1, q3 = send(q2, "b", 2), send(q1, "b", 1), send(q3, "b", 3)
    partial = own + (q1.astype(F32) + q3.astype(F32)) + q2.astype(F32)
    w = [partial[s].astype(BF) for s in range(4)]
    w2, w1, w3 = send(w[2], "z", 2), send(w[1], "z", 1), send(w[3], "z", 3)
    gradient = partial[0] + (w1.astype(F32) + w3.astype(F32)) + w2.astype(F32)

    squares = jnp.sum(gradient * gradient)
    total = jnp.sum(lax.all_to_all(jnp.broadcast_to(squares, (count,)), DP, 0, 0, tiled=True))
    clip = jnp.minimum(1.0, jnp.sqrt(jnp.float32(count * width)) / (jnp.sqrt(total) + 1e-06))
    clipped = clip * gradient.reshape(width)
    m_new = 0.5 * m_prev + 0.5 * clipped
    v_new = 0.95 * v_prev + 0.05 * clipped * clipped
    direction = m_new / (1.0 - 0.5**20) / (jnp.sqrt(v_new / (1.0 - 0.95**20)) + 1e-08)
    master_new = master - 0.05 * (direction + 0.1 * master)

    piece = master_new.astype(BF).reshape(1, rows, 128)
    for axis in ("z", "b"):
        got = {s: send(piece, axis, s) for s in (2, 1, 3)}
        piece = jnp.concatenate([piece, got[3], got[2], got[1]])
    got = {0: piece}
    for s in (2, 1, 3):
        got[(4 - s) % 4] = send(piece, "a", s)
    other = {0: send(got[0], "core")}
    out = place([(mine[0], got[0]), (theirs[0], other[0])], None)
    got[2], out = lax.optimization_barrier((got[2], out))
    other[2] = send(got[2], "core")
    out = place([(mine[2], got[2]), (theirs[2], other[2])], out)
    got[3], out = lax.optimization_barrier((got[3], out))
    other[3] = send(got[3], "core")
    other[1] = send(got[1], "core")
    out = place([(mine[3], got[3]), (mine[1], got[1]), (theirs[3], other[3])], out)
    out = place([(theirs[1], other[1])], out)
    return (master_new, m_new, v_new, out.reshape(count * width))


def solution(mesh):
    finer = Mesh(mesh.devices.reshape(4, 4, 4, 2), DP)
    placed = (P(DP, None), P(DP), P(DP, None), P(DP, None), P())
    return jax.shard_map(
        step, mesh=finer, in_specs=placed, out_specs=(P(DP), P(DP), P(DP), P()), check_vma=False
    )
```

```python
import jax
import jax.numpy as jnp
from jax import lax
from jax.experimental import pallas as pl
from jax.experimental.pallas import tpu as pltpu
from jax.sharding import Mesh
from jax.sharding import PartitionSpec as P

DP = ("z", "y", "x", "core")
BF = jnp.bfloat16
F32 = jnp.float32


def coords(d):
    return d // 32, d // 8 % 4, d // 2 % 4, d % 2


def shard_of(z, y, x, c):
    return ((z * 4 + y) * 4 + x) * 2 + c


def perm(axis, s):
    pairs = []
    for d in range(128):
        z, y, x, c = coords(d)
        if axis == "core":
            c = 1 - c
        elif axis == "z":
            z = (z + s) % 4
        elif (axis == "a") == (c == 0):
            x = (x + s) % 4
        else:
            y = (y + s) % 4
        pairs.append((d, shard_of(z, y, x, c)))
    return pairs


def send(value, axis, s=1):
    return lax.ppermute(value, DP, perm(axis, s))


def table(c, z, y, x, s):
    i = jnp.arange(16, dtype=jnp.int32)
    rb, rz = i // 4, i % 4
    zz = (z + rz) % 4
    on_0 = shard_of(zz, (y + rb) % 4, (x + s) % 4, 0)
    on_1 = shard_of(zz, (y + s) % 4, (x + rb) % 4, 1)
    return jnp.where(c == 0, on_0, on_1).astype(jnp.int32)


def cost(flops, nbytes):
    return pl.CostEstimate(flops=flops, transcendentals=0, bytes_accessed=nbytes)


def call(body, t, operands, outs, scratch, flops, nbytes, aliases=None, spaces=None, limit=8):
    vmem = pl.BlockSpec(memory_space=pltpu.VMEM)
    hbm = pl.BlockSpec(memory_space=pltpu.HBM)
    spaces = spaces or [True] * len(operands)
    operands = [pltpu.with_memory_space_constraint(o, pltpu.VMEM if v else pltpu.HBM) for o, v in zip(operands, spaces)]
    return pl.pallas_call(
        body,
        grid_spec=pltpu.PrefetchScalarGridSpec(
            num_scalar_prefetch=1,
            grid=(1,),
            in_specs=[vmem if v else hbm for v in spaces],
            out_specs=[hbm if isinstance(o, jax.ShapeDtypeStruct) else vmem for o in outs],
            scratch_shapes=scratch,
        ),
        out_shape=outs,
        input_output_aliases=aliases or {},
        cost_estimate=cost(flops, nbytes),
        compiler_params=pltpu.CompilerParams(vmem_limit_bytes=limit * 2**20),
    )(t, *operands)


def fetch(t, g, dtype):
    _, rows, lanes = g.shape
    whole = dtype == g.dtype

    def body(t_ref, g_ref, *refs):
        outs, (*buf, sem) = refs[:4], refs[4:]
        to = [outs[i // 16].at[i % 16] if whole else buf[0].at[i] for i in range(64)]
        copies = [pltpu.make_async_copy(g_ref.at[t_ref[i]], to[i], sem.at[i]) for i in range(64)]
        for copy in copies:
            copy.start()
        for i, copy in enumerate(copies):
            copy.wait()
            if not whole:
                outs[i // 16][i % 16] = buf[0][i].astype(dtype)

    scratch = [] if whole else [pltpu.VMEM((64, rows, lanes), g.dtype)]
    n = 64 * rows * lanes
    return call(
        body,
        t,
        (g,),
        [pltpu.VMEM((16, rows, lanes), dtype)] * 4,
        scratch + [pltpu.SemaphoreType.DMA((64,))],
        n,
        6 * n,
        spaces=[False],
        limit=2 if whole else 10,
    )


def sum_piece(parts, split=False):
    n, rows, lanes = parts[0].shape
    m = len(parts)

    def body(t_ref, *refs):
        ins, outs = refs[:m], refs[m:]
        each = n // len(outs)

        for q, o in enumerate(outs):

            @pl.loop(0, each)
            def _(i, q=q, o=o):
                value = ins[0][q * each + i].astype(F32)
                for r in ins[1:]:
                    value = value + r[q * each + i].astype(F32)
                o[i] = value.astype(o.dtype)

    if split:
        outs = [pltpu.VMEM((n // 4, rows, lanes), F32)] + [pltpu.VMEM((n // 4, rows, lanes), BF)] * 3
    else:
        outs = [pltpu.VMEM((n, rows, lanes), BF)]
    size = n * rows * lanes
    got = call(body, jnp.zeros((1,), jnp.int32), parts, outs, [], m * size, (6 + 2 * m) * size)
    return got if split else got[0]


def place(pairs, out):
    k = len(pairs)
    n, rows, lanes = pairs[0][1].shape

    def body(t_ref, *refs):
        o, sem = refs[-2:]
        copies = [
            pltpu.make_async_copy(refs[j].at[i], o.at[t_ref[j * n + i]], sem.at[j * n + i])
            for j in range(k)
            for i in range(n)
        ]
        for copy in copies:
            copy.start()
        for copy in copies:
            copy.wait()

    t = jnp.concatenate([p[0] for p in pairs])
    operands = [p[1] for p in pairs] + ([] if out is None else [out])
    nbytes = 4 * k * n * rows * lanes
    return call(
        body,
        t,
        operands,
        [jax.ShapeDtypeStruct((128, rows, lanes), BF)],
        [pltpu.SemaphoreType.DMA((k * n,))],
        nbytes,
        nbytes,
        {} if out is None else {k + 1: 0},
        [True] * k + [False] * (0 if out is None else 1),
    )[0]


def total_piece(own, from1, from2, from3, copies):
    n, rows, lanes = own.shape

    def body(t_ref, w, x1, x2, x3, g, squares):
        sums = []
        for r in range(n):

            def step(i, acc, r=r):
                at = pl.ds(i * 16, 16)
                even = w[r, at].astype(F32) + x2[(r + 2) % n, at].astype(F32)
                odd = x1[(r + 1) % n, at].astype(F32) + x3[(r + 3) % n, at].astype(F32)
                value = even + odd
                g[r, at] = value
                return acc + value * value

            sums.append(lax.fori_loop(0, rows // 16, step, jnp.zeros((16, lanes), F32)))
        acc = (sums[0] + sums[2]) + (sums[1] + sums[3])
        squares[...] = jnp.broadcast_to(jnp.sum(acc), squares.shape)

    size = n * rows * lanes
    outs = [pltpu.VMEM((n, rows, lanes), F32), pltpu.VMEM((copies, 8, lanes), F32)]
    return call(body, jnp.zeros((1,), jnp.int32), (own, from1, from2, from3), outs, [], 6 * size, 12 * size)


def adam(master, m_prev, v_prev, gradient, clip):
    clipped = clip * gradient
    m_new = 0.5 * m_prev + 0.5 * clipped
    v_new = 0.95 * v_prev + 0.05 * clipped * clipped
    direction = m_new / (1.0 - 0.5**20) / (jnp.sqrt(v_new / (1.0 - 0.95**20)) + 1e-08)
    return master - 0.05 * (direction + 0.1 * master), m_new, v_new


def updated_piece(gradient, states, squares, flat):
    n, rows, lanes = gradient.shape

    def body(t_ref, g, *refs):
        state, part, piece, clip_ref = refs[:n], refs[n], refs[n + 1], refs[n + 2]
        total = part[0]
        for i in range(1, part.shape[0]):
            total = total + part[i]
        clip = jnp.minimum(1.0, jnp.sqrt(jnp.float32(flat)) / (jnp.sqrt(total) + 1e-06))
        clip_ref[...] = clip
        clip = jnp.concatenate([clip, clip])
        for r in range(n):

            @pl.loop(0, rows // 16)
            def _(i, r=r):
                at = pl.ds(i * 16, 16)
                high, low, m, v = (state[r][k, at].astype(F32) for k in range(4))
                piece[r, at] = adam(high + low, m, v, g[r, at], clip)[0].astype(BF)

    size = n * rows * lanes
    outs = [pltpu.VMEM((n, rows, lanes), BF), pltpu.VMEM((8, lanes), F32)]
    return call(body, jnp.zeros((1,), jnp.int32), (gradient, *states, squares), outs, [], 20 * size, 14 * size)


def packed_moments(m_old, v_old):
    def body(t_ref, m, v, o):
        o[0] = m[...].astype(BF)
        o[1] = v[...].astype(BF)

    n = 2 * m_old.size
    outs = [pltpu.VMEM((2, *m_old.shape), BF)]
    return call(body, jnp.zeros((1,), jnp.int32), (m_old, v_old), outs, [], n, 6 * n)[0]


def old_moments(device, old_bounds, m_old, v_old, before, after, master):
    rows, lanes = master.shape
    top = 392
    reach = top + m_old.shape[0] + rows // 2 + 8
    where = jnp.concatenate([old_bounds, device[None].astype(jnp.int32)])
    last = old_bounds.shape[0]

    def body(t_ref, m, v, b, a, w, m_out, v_out, state, buf):
        d = t_ref[last]
        start = d * (rows * lanes)
        first = t_ref[d]
        end = t_ref[d + 1]
        starts = (t_ref[jnp.maximum(d - 1, 0)], first, end)
        offsets = [start - s + top * lanes for s in starts]
        for k, (old, out) in enumerate(((m, m_out), (v, v_out))):
            held = pl.ds(top, m_old.shape[0])
            buf[0, held] = b[k].astype(F32)
            buf[1, held] = old[...]
            buf[2, held] = a[k].astype(F32)

            @pl.loop(0, rows // 32)
            def _(i, k=k, out=out):
                lane = lax.broadcasted_iota(jnp.int32, (32, lanes), 1)
                row = lax.broadcasted_iota(jnp.int32, (32, lanes), 0)
                position = start + i * (32 * lanes) + row * lanes + lane
                parts = []
                for j, offset in enumerate(offsets):
                    q = offset // lanes + i * 32
                    r = offset % lanes
                    back = (lanes - r) % lanes
                    here = pltpu.roll(buf[j, pl.ds(q, 32)], back, 1)
                    then = pltpu.roll(buf[j, pl.ds(q + 1, 32)], back, 1)
                    parts.append(jnp.where(lane < lanes - r, here, then))
                value = jnp.where(position < first, parts[0], jnp.where(position >= end, parts[2], parts[1]))
                at = pl.ds(i * 32, 32)
                out[at] = value
                state[2 + k, at] = value.astype(BF)

        high = w[...].astype(BF)
        state[0] = high
        state[1] = (w[...] - high.astype(F32)).astype(BF)

    size = rows * lanes
    outs = [pltpu.VMEM((rows, lanes), F32)] * 2 + [pltpu.VMEM((4, rows, lanes), BF)]
    return call(
        body,
        where,
        (m_old, v_old, before, after, master),
        outs,
        [pltpu.VMEM((3, reach, lanes), F32)],
        40 * size,
        40 * size,
    )


def shifted(value, steps):
    leading, last = (max(0, -steps), min(128, 128 - steps))
    return lax.ppermute(value, DP, [(source, source + steps) for source in range(leading, last)])


def step(grads, master, m_old, v_old, old_bounds):
    count = 128
    width = master.shape[0]
    rows = width // 128
    device = lax.axis_index(DP)
    z, y, x, c = coords(device)
    mine = [table(c, z, y, x, s) for s in range(4)]
    theirs = [table(1 - c, z, y, x, s) for s in range(4)]
    g = grads[0].reshape(128, rows, 128)

    order = (2, 1, 3, 0)
    given = fetch(jnp.concatenate([theirs[s] for s in order]), g, BF)
    swapped = {s: send(v, "core") for s, v in zip(order, given)}
    kept = fetch(jnp.concatenate([mine[s] for s in order]), g, F32)
    kept = dict(zip(order, kept))
    ringed = {}
    pieces = {}
    for s in (2, 1, 3):
        pieces[s] = sum_piece((kept[s], swapped[s]))
        ringed[s] = send(pieces[s], "a", s)
    master_tiles = master.reshape(rows, 128)
    m_tiles, v_tiles = m_old[0].reshape(-1, 128), v_old[0].reshape(-1, 128)
    packed = packed_moments(m_tiles, v_tiles)
    before = shifted(packed, 1)
    after = shifted(packed, -1)
    m_prev, v_prev, state = old_moments(device, old_bounds, m_tiles, v_tiles, before, after, master_tiles)
    states = [state] + [None] * 3
    for s in (2, 1, 3):
        states[4 - s] = send(state, "z", s)
    own, q1, q2, q3 = sum_piece((kept[0], swapped[0], ringed[1], ringed[2], ringed[3]), split=True)
    q2, q1, q3 = send(q2, "b", 2), send(q1, "b", 1), send(q3, "b", 3)
    partial = sum_piece((own, q1, q2, q3))
    w2, w1, w3 = send(partial, "z", 2), send(partial, "z", 1), send(partial, "z", 3)
    gradient, squares = total_piece(partial, w1, w2, w3, 32)
    squares = lax.all_to_all(squares, ("y", "x", "core"), 0, 0, tiled=True)
    piece, clip = updated_piece(gradient, states, squares, count * width)
    new = adam(master_tiles, m_prev, v_prev, gradient[0], clip[0, 0])
    master_new, m_new, v_new = (value.reshape(width) for value in new)

    got = {s: send(piece, "b", s) for s in (2, 1, 3)}
    piece = jnp.concatenate([piece, got[3], got[2], got[1]])
    got = {0: piece}
    for s in (2, 1, 3):
        got[(4 - s) % 4] = send(piece, "a", s)
    other = {0: send(got[0], "core")}
    out = place([(mine[0], got[0]), (theirs[0], other[0])], None)
    got[2], out = lax.optimization_barrier((got[2], out))
    other[2] = send(got[2], "core")
    out = place([(mine[2], got[2]), (theirs[2], other[2])], out)
    got[3], out = lax.optimization_barrier((got[3], out))
    other[3] = send(got[3], "core")
    other[1] = send(got[1], "core")
    out = place([(mine[3], got[3]), (mine[1], got[1])], out)
    out = place([(theirs[3], other[3]), (theirs[1], other[1])], out)
    return (master_new, m_new, v_new, out.reshape(count * width))


def solution(mesh):
    finer = Mesh(mesh.devices.reshape(4, 4, 4, 2), DP)
    placed = (P(DP, None), P(DP), P(DP, None), P(DP, None), P())
    return jax.shard_map(step, mesh=finer, in_specs=placed, out_specs=(P(DP), P(DP), P(DP), P()), check_vma=False)
```

```python
import jax
import jax.numpy as jnp
from jax import lax
from jax.experimental import pallas as pl
from jax.experimental.pallas import tpu as pltpu
from jax.sharding import Mesh
from jax.sharding import PartitionSpec as P

DP = ("z", "y", "x", "core")
BF = jnp.bfloat16
F32 = jnp.float32


def coords(d):
    return d // 32, d // 8 % 4, d // 2 % 4, d % 2


def shard_of(z, y, x, c):
    return ((z * 4 + y) * 4 + x) * 2 + c


def perm(axis, s):
    pairs = []
    for d in range(128):
        z, y, x, c = coords(d)
        if axis == "core":
            c = 1 - c
        elif axis == "z":
            z = (z + s) % 4
        elif (axis == "a") == (c == 0):
            x = (x + s) % 4
        else:
            y = (y + s) % 4
        pairs.append((d, shard_of(z, y, x, c)))
    return pairs


def send(value, axis, s=1):
    return lax.ppermute(value, DP, perm(axis, s))


def table(c, z, y, x, s):
    i = jnp.arange(16, dtype=jnp.int32)
    rb, rz = i // 4, i % 4
    zz = (z + rz) % 4
    on_0 = shard_of(zz, (y + rb) % 4, (x + s) % 4, 0)
    on_1 = shard_of(zz, (y + s) % 4, (x + rb) % 4, 1)
    return jnp.where(c == 0, on_0, on_1).astype(jnp.int32)


def cost(flops, nbytes):
    return pl.CostEstimate(flops=flops, transcendentals=0, bytes_accessed=nbytes)


def call(body, t, operands, outs, scratch, flops, nbytes, aliases=None, spaces=None, limit=8):
    vmem = pl.BlockSpec(memory_space=pltpu.VMEM)
    hbm = pl.BlockSpec(memory_space=pltpu.HBM)
    spaces = spaces or [True] * len(operands)
    operands = [pltpu.with_memory_space_constraint(o, pltpu.VMEM if v else pltpu.HBM) for o, v in zip(operands, spaces)]
    return pl.pallas_call(
        body,
        grid_spec=pltpu.PrefetchScalarGridSpec(
            num_scalar_prefetch=1,
            grid=(1,),
            in_specs=[vmem if v else hbm for v in spaces],
            out_specs=[hbm if isinstance(o, jax.ShapeDtypeStruct) else vmem for o in outs],
            scratch_shapes=scratch,
        ),
        out_shape=outs,
        input_output_aliases=aliases or {},
        cost_estimate=cost(flops, nbytes),
        compiler_params=pltpu.CompilerParams(vmem_limit_bytes=limit * 2**20),
    )(t, *operands)


def fetch(g, *pieces):
    _, rows, lanes = g.shape
    n = 16
    kept = [dtype == g.dtype for _, dtype in pieces]
    m = len(pieces)

    def body(t_ref, g_ref, *refs):
        outs, rest = refs[:m], refs[m:]
        sem, buf = rest[-1], rest[0]
        copies = []
        for k in range(m):
            slot = sum(not v for v in kept[:k]) * n
            for i in range(n):
                to = outs[k].at[i] if kept[k] else buf.at[slot + i]
                copies.append((k, i, slot + i, pltpu.make_async_copy(g_ref.at[t_ref[k * n + i]], to, sem.at[k * n + i])))
        for *_, copy in copies:
            copy.start()
        for k, i, at, copy in copies:
            copy.wait()
            if not kept[k]:
                outs[k][i] = buf[at].astype(outs[k].dtype)

    converted = m - sum(kept)
    scratch = [pltpu.VMEM((converted * n, rows, lanes), g.dtype)] if converted else []
    size = m * n * rows * lanes
    return call(
        body,
        jnp.concatenate([t for t, _ in pieces]),
        (g,),
        [pltpu.VMEM((n, rows, lanes), dtype) for _, dtype in pieces],
        scratch + [pltpu.SemaphoreType.DMA((m * n,))],
        size,
        6 * size,
        spaces=[False],
        limit=2 + 2 * converted,
    )


def sum_piece(parts, split=False):
    n, rows, lanes = parts[0].shape
    m = len(parts)

    def body(t_ref, *refs):
        ins, outs = refs[:m], refs[m:]
        each = n // len(outs)

        for q, o in enumerate(outs):

            @pl.loop(0, each)
            def _(i, q=q, o=o):
                value = ins[0][q * each + i].astype(F32)
                for r in ins[1:]:
                    value = value + r[q * each + i].astype(F32)
                o[i] = value.astype(o.dtype)

    if split:
        outs = [pltpu.VMEM((n // 4, rows, lanes), F32)] + [pltpu.VMEM((n // 4, rows, lanes), BF)] * 3
    else:
        outs = [pltpu.VMEM((n, rows, lanes), BF)]
    size = n * rows * lanes
    got = call(body, jnp.zeros((1,), jnp.int32), parts, outs, [], m * size, (6 + 2 * m) * size)
    return got if split else got[0]


def place(pairs, out):
    k = len(pairs)
    n, rows, lanes = pairs[0][1].shape

    def body(t_ref, *refs):
        o, sem = refs[-2:]
        copies = [
            pltpu.make_async_copy(refs[j].at[i], o.at[t_ref[j * n + i]], sem.at[j * n + i])
            for j in range(k)
            for i in range(n)
        ]
        for copy in copies:
            copy.start()
        for copy in copies:
            copy.wait()

    t = jnp.concatenate([p[0] for p in pairs])
    operands = [p[1] for p in pairs] + ([] if out is None else [out])
    nbytes = 4 * k * n * rows * lanes
    return call(
        body,
        t,
        operands,
        [jax.ShapeDtypeStruct((128, rows, lanes), BF)],
        [pltpu.SemaphoreType.DMA((k * n,))],
        nbytes,
        nbytes,
        {} if out is None else {k + 1: 0},
        [True] * k + [False] * (0 if out is None else 1),
    )[0]


def total_piece(own, from1, from2, from3, copies):
    n, rows, lanes = own.shape

    def body(t_ref, w, x1, x2, x3, g, squares):
        sums = []
        for r in range(n):

            def step(i, acc, r=r):
                at = pl.ds(i * 16, 16)
                even = w[r, at].astype(F32) + x2[(r + 2) % n, at].astype(F32)
                odd = x1[(r + 1) % n, at].astype(F32) + x3[(r + 3) % n, at].astype(F32)
                value = even + odd
                g[r, at] = value
                return acc + value * value

            sums.append(lax.fori_loop(0, rows // 16, step, jnp.zeros((16, lanes), F32)))
        acc = (sums[0] + sums[2]) + (sums[1] + sums[3])
        squares[...] = jnp.broadcast_to(jnp.sum(acc), squares.shape)

    size = n * rows * lanes
    outs = [pltpu.VMEM((n, rows, lanes), F32), pltpu.VMEM((copies, 8, lanes), F32)]
    return call(body, jnp.zeros((1,), jnp.int32), (own, from1, from2, from3), outs, [], 6 * size, 12 * size)


def adam(master, m_prev, v_prev, gradient, clip):
    clipped = clip * gradient
    m_new = 0.5 * m_prev + 0.5 * clipped
    v_new = 0.95 * v_prev + 0.05 * clipped * clipped
    direction = m_new / (1.0 - 0.5**20) / (jnp.sqrt(v_new / (1.0 - 0.95**20)) + 1e-08)
    return master - 0.05 * (direction + 0.1 * master), m_new, v_new


def updated_piece(gradient, states, squares, flat):
    n, rows, lanes = gradient.shape

    def body(t_ref, g, *refs):
        state, part, piece, clip_ref = refs[:n], refs[n], refs[n + 1], refs[n + 2]
        total = part[0]
        for i in range(1, part.shape[0]):
            total = total + part[i]
        clip = jnp.minimum(1.0, jnp.sqrt(jnp.float32(flat)) / (jnp.sqrt(total) + 1e-06))
        clip_ref[...] = clip
        clip = jnp.concatenate([clip, clip])
        for r in range(n):

            @pl.loop(0, rows // 16)
            def _(i, r=r):
                at = pl.ds(i * 16, 16)
                high, low, m, v = (state[r][k, at].astype(F32) for k in range(4))
                piece[r, at] = adam(high + low, m, v, g[r, at], clip)[0].astype(BF)

    size = n * rows * lanes
    outs = [pltpu.VMEM((n, rows, lanes), BF), pltpu.VMEM((8, lanes), F32)]
    return call(body, jnp.zeros((1,), jnp.int32), (gradient, *states, squares), outs, [], 20 * size, 14 * size)


def moved_rows(end, half, lanes, total):
    return jnp.minimum(jnp.maximum(end - half * lanes, 0) // lanes, total - half - 8)


def packed_moments(where, m_old, v_old, half):
    total, lanes = m_old.shape
    last = where.shape[0] - 1

    def body(t_ref, m, v, up, down):
        d = t_ref[last]
        q = moved_rows(t_ref[d + 1] - t_ref[d], half, lanes, total)
        for k, old in enumerate((m, v)):
            up[k] = old[pl.ds(q, half + 8)].astype(BF)
            down[k] = old[pl.ds(0, half)].astype(BF)

    n = 4 * half * lanes
    outs = [pltpu.VMEM((2, half + 8, lanes), BF), pltpu.VMEM((2, half, lanes), BF)]
    return call(body, where, (m_old, v_old), outs, [], n, 6 * n)


def old_moments(where, m_old, v_old, before, after, passed, master):
    rows, lanes = master.shape
    total = m_old.shape[0]
    half = rows // 2
    top = 392
    reach = top + total + half + 8
    last = where.shape[0] - 1

    def body(t_ref, m, v, b, a, p, w, m_out, v_out, state, buf):
        d = t_ref[last]
        start = d * (rows * lanes)
        first = t_ref[d]
        end = t_ref[d + 1]
        ahead = t_ref[jnp.maximum(d - 1, 0)]
        q = moved_rows(first - ahead, half, lanes, total)
        offsets = [start - s + top * lanes for s in (ahead + q * lanes, first, end)]
        for k, (old, out) in enumerate(((m, m_out), (v, v_out))):
            buf[0, pl.ds(top, half + 8)] = b[k].astype(F32)
            buf[1, pl.ds(top, total)] = old[...]

            @pl.when(d % 2 == 0)
            def _(k=k):
                buf[2, pl.ds(top, half)] = a[k].astype(F32)

            @pl.when(d % 2 == 1)
            def _(k=k):
                buf[2, pl.ds(top, half)] = p[k].astype(F32)

            def part(j, i):
                lane = lax.broadcasted_iota(jnp.int32, (32, lanes), 1)
                at = offsets[j] // lanes + i * 32
                r = offsets[j] % lanes
                back = (lanes - r) % lanes
                here = pltpu.roll(buf[j, pl.ds(at, 32)], back, 1)
                then = pltpu.roll(buf[j, pl.ds(at + 1, 32)], back, 1)
                return jnp.where(lane < lanes - r, here, then)

            for low in (True, False):

                @pl.loop(0, half // 32)
                def _(step, k=k, out=out, low=low):
                    i = step if low else step + half // 32
                    lane = lax.broadcasted_iota(jnp.int32, (32, lanes), 1)
                    row = lax.broadcasted_iota(jnp.int32, (32, lanes), 0)
                    position = start + i * (32 * lanes) + row * lanes + lane
                    if low:
                        value = jnp.where(position < first, part(0, i), part(1, i))
                    else:
                        value = jnp.where(position >= end, part(2, i), part(1, i))
                    at = pl.ds(i * 32, 32)
                    out[at] = value
                    state[2 + k, at] = value.astype(BF)

        high = w[...].astype(BF)
        state[0] = high
        state[1] = (w[...] - high.astype(F32)).astype(BF)

    size = rows * lanes
    outs = [pltpu.VMEM((rows, lanes), F32)] * 2 + [pltpu.VMEM((4, rows, lanes), BF)]
    return call(
        body,
        where,
        (m_old, v_old, before, after, passed, master),
        outs,
        [pltpu.VMEM((3, reach, lanes), F32)],
        40 * size,
        40 * size,
    )


def step(grads, master, m_old, v_old, old_bounds):
    count = 128
    width = master.shape[0]
    rows = width // 128
    device = lax.axis_index(DP)
    z, y, x, c = coords(device)
    mine = [table(c, z, y, x, s) for s in range(4)]
    theirs = [table(1 - c, z, y, x, s) for s in range(4)]
    g = grads[0].reshape(128, rows, 128)

    given, kept, swapped, pieces, ringed = {}, {}, {}, {}, {}
    (given[2],) = fetch(g, (theirs[2], BF))
    swapped[2] = send(given[2], "core")
    kept[2], given[1], given[3] = fetch(g, (mine[2], F32), (theirs[1], BF), (theirs[3], BF))
    swapped[1] = send(given[1], "core")
    swapped[3] = send(given[3], "core")
    kept[1], kept[3] = fetch(g, (mine[1], F32), (mine[3], F32))
    given[0], kept[0] = fetch(g, (theirs[0], BF), (mine[0], F32))
    swapped[0] = send(given[0], "core")
    for s in (2, 1, 3):
        pieces[s] = sum_piece((kept[s], swapped[s]))
        ringed[s] = send(pieces[s], "a", s)
    master_tiles = master.reshape(rows, 128)
    m_tiles, v_tiles = m_old[0].reshape(-1, 128), v_old[0].reshape(-1, 128)
    where = jnp.concatenate([old_bounds, device[None].astype(jnp.int32)])
    up, down = packed_moments(where, m_tiles, v_tiles, rows // 2)
    before = lax.ppermute(up, DP, [(d, d + 1) for d in range(127)])
    after = send(down, "core")
    passed = lax.ppermute(after, DP, [(d, d - 2) for d in range(3, 128, 2)])
    m_prev, v_prev, state = old_moments(where, m_tiles, v_tiles, before, after, passed, master_tiles)
    states = [state] + [None] * 3
    for s in (2, 1, 3):
        states[4 - s] = send(state, "z", s)
    own, q1, q2, q3 = sum_piece((kept[0], swapped[0], ringed[1], ringed[2], ringed[3]), split=True)
    q2, q1, q3 = send(q2, "b", 2), send(q1, "b", 1), send(q3, "b", 3)
    partial = sum_piece((own, q1, q2, q3))
    w2, w1, w3 = send(partial, "z", 2), send(partial, "z", 1), send(partial, "z", 3)
    gradient, squares = total_piece(partial, w1, w2, w3, 32)
    squares = lax.all_to_all(squares, ("y", "x", "core"), 0, 0, tiled=True)
    piece, clip = updated_piece(gradient, states, squares, count * width)
    new = adam(master_tiles, m_prev, v_prev, gradient[0], clip[0, 0])
    master_new, m_new, v_new = (value.reshape(width) for value in new)

    got = {s: send(piece, "b", s) for s in (2, 1, 3)}
    piece = jnp.concatenate([piece, got[3], got[2], got[1]])
    got = {0: piece}
    for s in (2, 1, 3):
        got[(4 - s) % 4] = send(piece, "a", s)
    other = {0: send(got[0], "core")}
    out = place([(mine[0], got[0]), (theirs[0], other[0])], None)
    got[2], out = lax.optimization_barrier((got[2], out))
    other[2] = send(got[2], "core")
    out = place([(mine[2], got[2]), (theirs[2], other[2])], out)
    got[3], out = lax.optimization_barrier((got[3], out))
    other[3] = send(got[3], "core")
    other[1] = send(got[1], "core")
    out = place([(mine[3], got[3]), (mine[1], got[1])], out)
    out = place([(theirs[3], other[3]), (theirs[1], other[1])], out)
    return (master_new, m_new, v_new, out.reshape(count * width))


def solution(mesh):
    finer = Mesh(mesh.devices.reshape(4, 4, 4, 2), DP)
    placed = (P(DP, None), P(DP), P(DP, None), P(DP, None), P())
    return jax.shard_map(step, mesh=finer, in_specs=placed, out_specs=(P(DP), P(DP), P(DP), P()), check_vma=False)
```

```python
import jax
import jax.numpy as jnp
from jax import lax
from jax.experimental import pallas as pl
from jax.experimental.pallas import tpu as pltpu
from jax.sharding import Mesh
from jax.sharding import PartitionSpec as P

DP = ("z", "y", "x", "core")
BF = jnp.bfloat16
F32 = jnp.float32


def coords(d):
    return d // 32, d // 8 % 4, d // 2 % 4, d % 2


def shard_of(z, y, x, c):
    return ((z * 4 + y) * 4 + x) * 2 + c


def perm(axis, s):
    pairs = []
    for d in range(128):
        z, y, x, c = coords(d)
        if axis == "core":
            c = 1 - c
        elif axis == "z":
            z = (z + s) % 4
        elif (axis == "a") == (c == 0):
            x = (x + s) % 4
        else:
            y = (y + s) % 4
        pairs.append((d, shard_of(z, y, x, c)))
    return pairs


def send(value, axis, s=1):
    return lax.ppermute(value, DP, perm(axis, s))


def table(c, z, y, x, s):
    i = jnp.arange(16, dtype=jnp.int32)
    rb, rz = i // 4, i % 4
    zz = (z + rz) % 4
    on_0 = shard_of(zz, (y + rb) % 4, (x + s) % 4, 0)
    on_1 = shard_of(zz, (y + s) % 4, (x + rb) % 4, 1)
    return jnp.where(c == 0, on_0, on_1).astype(jnp.int32)


def cost(flops, nbytes):
    return pl.CostEstimate(flops=flops, transcendentals=0, bytes_accessed=nbytes)


def call(body, t, operands, outs, scratch, flops, nbytes, aliases=None, spaces=None, limit=8):
    vmem = pl.BlockSpec(memory_space=pltpu.VMEM)
    hbm = pl.BlockSpec(memory_space=pltpu.HBM)
    spaces = spaces or [True] * len(operands)
    operands = [pltpu.with_memory_space_constraint(o, pltpu.VMEM if v else pltpu.HBM) for o, v in zip(operands, spaces)]
    return pl.pallas_call(
        body,
        grid_spec=pltpu.PrefetchScalarGridSpec(
            num_scalar_prefetch=1,
            grid=(1,),
            in_specs=[vmem if v else hbm for v in spaces],
            out_specs=[hbm if isinstance(o, jax.ShapeDtypeStruct) else vmem for o in outs],
            scratch_shapes=scratch,
        ),
        out_shape=outs,
        input_output_aliases=aliases or {},
        cost_estimate=cost(flops, nbytes),
        compiler_params=pltpu.CompilerParams(vmem_limit_bytes=limit * 2**20),
    )(t, *operands)


def fetch(g, *pieces):
    _, rows, lanes = g.shape
    n = 16
    kept = [dtype == g.dtype for _, dtype in pieces]
    m = len(pieces)

    def body(t_ref, g_ref, *refs):
        outs, rest = refs[:m], refs[m:]
        sem, buf = rest[-1], rest[0]
        copies = []
        for k in range(m):
            slot = sum(not v for v in kept[:k]) * n
            for i in range(n):
                to = outs[k].at[i] if kept[k] else buf.at[slot + i]
                copies.append((k, i, slot + i, pltpu.make_async_copy(g_ref.at[t_ref[k * n + i]], to, sem.at[k * n + i])))
        for *_, copy in copies:
            copy.start()
        for k, i, at, copy in copies:
            copy.wait()
            if not kept[k]:
                outs[k][i] = buf[at].astype(outs[k].dtype)

    converted = m - sum(kept)
    scratch = [pltpu.VMEM((converted * n, rows, lanes), g.dtype)] if converted else []
    size = m * n * rows * lanes
    return call(
        body,
        jnp.concatenate([t for t, _ in pieces]),
        (g,),
        [pltpu.VMEM((n, rows, lanes), dtype) for _, dtype in pieces],
        scratch + [pltpu.SemaphoreType.DMA((m * n,))],
        size,
        6 * size,
        spaces=[False],
        limit=2 + 2 * converted,
    )


def sum_piece(parts, kinds):
    rows, lanes = parts[0][0][0].shape[1:]
    operands = [array for part in parts for array, _, _ in part]

    def sources(base):
        at = 0
        for part in parts:
            begin = 0
            for k, (_, first, count) in enumerate(part):
                if begin <= base < begin + count:
                    yield at + k, first + base - begin
                begin += count
            at += len(part)

    def body(t_ref, *refs):
        ins, outs = refs[: len(operands)], refs[len(operands) :]
        base = 0
        for o, (count, _) in zip(outs, kinds):
            where = list(sources(base))

            @pl.loop(0, count)
            def _(i, o=o, where=where):
                value = None
                for k, first in where:
                    term = ins[k][first + i].astype(F32)
                    value = term if value is None else value + term
                o[i] = value.astype(o.dtype)

            base += count

    size = sum(count for count, _ in kinds) * rows * lanes
    outs = [pltpu.VMEM((count, rows, lanes), dtype) for count, dtype in kinds]
    return call(body, jnp.zeros((1,), jnp.int32), operands, outs, [], len(parts) * size, (4 + 2 * len(parts)) * size)


def joined(first, second):
    def body(t_ref, a, b, o):
        o[: a.shape[0]] = a[...]
        o[a.shape[0] :] = b[...]

    shape = (first.shape[0] + second.shape[0], *first.shape[1:])
    n = first.size + second.size
    outs = [pltpu.VMEM(shape, first.dtype)]
    return call(body, jnp.zeros((1,), jnp.int32), (first, second), outs, [], n, 4 * n)[0]


def place(pairs, out):
    k = len(pairs)
    n, rows, lanes = pairs[0][1].shape

    def body(t_ref, *refs):
        o, sem = refs[-2:]
        copies = [
            pltpu.make_async_copy(refs[j].at[i], o.at[t_ref[j * n + i]], sem.at[j * n + i])
            for j in range(k)
            for i in range(n)
        ]
        for copy in copies:
            copy.start()
        for copy in copies:
            copy.wait()

    t = jnp.concatenate([p[0] for p in pairs])
    operands = [p[1] for p in pairs] + ([] if out is None else [out])
    nbytes = 4 * k * n * rows * lanes
    return call(
        body,
        t,
        operands,
        [jax.ShapeDtypeStruct((128, rows, lanes), BF)],
        [pltpu.SemaphoreType.DMA((k * n,))],
        nbytes,
        nbytes,
        {} if out is None else {k + 1: 0},
        [True] * k + [False] * (0 if out is None else 1),
    )[0]


def total_piece(own, from1, from2, from3, copies):
    n, rows, lanes = own.shape

    def body(t_ref, w, x1, x2, x3, g, squares):
        sums = []
        for r in range(n):

            def step(i, acc, r=r):
                at = pl.ds(i * 16, 16)
                even = w[r, at].astype(F32) + x2[(r + 2) % n, at].astype(F32)
                odd = x1[(r + 1) % n, at].astype(F32) + x3[(r + 3) % n, at].astype(F32)
                value = even + odd
                g[r, at] = value
                return acc + value * value

            sums.append(lax.fori_loop(0, rows // 16, step, jnp.zeros((16, lanes), F32)))
        acc = (sums[0] + sums[2]) + (sums[1] + sums[3])
        squares[...] = jnp.broadcast_to(jnp.sum(acc), squares.shape)

    size = n * rows * lanes
    outs = [pltpu.VMEM((n, rows, lanes), F32), pltpu.VMEM((copies, 8, lanes), F32)]
    return call(body, jnp.zeros((1,), jnp.int32), (own, from1, from2, from3), outs, [], 6 * size, 12 * size)


def adam(master, m_prev, v_prev, gradient, clip):
    clipped = clip * gradient
    m_new = 0.5 * m_prev + 0.5 * clipped
    v_new = 0.95 * v_prev + 0.05 * clipped * clipped
    direction = m_new / (1.0 - 0.5**20) / (jnp.sqrt(v_new / (1.0 - 0.95**20)) + 1e-08)
    return master - 0.05 * (direction + 0.1 * master), m_new, v_new


def updated_piece(gradient, states, squares, flat):
    n, rows, lanes = gradient.shape

    def body(t_ref, g, *refs):
        state, part, piece, clip_ref = refs[:n], refs[n], refs[n + 1], refs[n + 2]
        total = part[0]
        for i in range(1, part.shape[0]):
            total = total + part[i]
        clip = jnp.minimum(1.0, jnp.sqrt(jnp.float32(flat)) / (jnp.sqrt(total) + 1e-06))
        clip_ref[...] = clip
        clip = jnp.concatenate([clip, clip])
        for r in range(n):

            @pl.loop(0, rows // 16)
            def _(i, r=r):
                at = pl.ds(i * 16, 16)
                high, low, m, v = (state[r][k, at].astype(F32) for k in range(4))
                piece[r, at] = adam(high + low, m, v, g[r, at], clip)[0].astype(BF)

    size = n * rows * lanes
    outs = [pltpu.VMEM((n, rows, lanes), BF), pltpu.VMEM((8, lanes), F32)]
    return call(body, jnp.zeros((1,), jnp.int32), (gradient, *states, squares), outs, [], 20 * size, 14 * size)


def moved_rows(end, half, lanes, total):
    return jnp.minimum(jnp.maximum(end - half * lanes, 0) // lanes, total - half - 8)


def packed_moments(where, m_old, v_old, half):
    total, lanes = m_old.shape
    last = where.shape[0] - 1

    def body(t_ref, m, v, up, down):
        d = t_ref[last]
        q = moved_rows(t_ref[d + 1] - t_ref[d], half, lanes, total)
        for k, old in enumerate((m, v)):
            up[k] = old[pl.ds(q, half + 8)].astype(BF)
            down[k] = old[pl.ds(0, half)].astype(BF)

    n = 4 * half * lanes
    outs = [pltpu.VMEM((2, half + 8, lanes), BF), pltpu.VMEM((2, half, lanes), BF)]
    return call(body, where, (m_old, v_old), outs, [], n, 6 * n)


def old_moments(where, m_old, v_old, before, after, passed, master):
    rows, lanes = master.shape
    total = m_old.shape[0]
    half = rows // 2
    top = 392
    reach = top + total + half + 8
    last = where.shape[0] - 1

    def body(t_ref, m, v, b, a, p, w, m_out, v_out, state, buf):
        d = t_ref[last]
        start = d * (rows * lanes)
        first = t_ref[d]
        end = t_ref[d + 1]
        ahead = t_ref[jnp.maximum(d - 1, 0)]
        q = moved_rows(first - ahead, half, lanes, total)
        offsets = [start - s + top * lanes for s in (ahead + q * lanes, first, end)]
        for k, (old, out) in enumerate(((m, m_out), (v, v_out))):
            buf[0, pl.ds(top, half + 8)] = b[k].astype(F32)
            buf[1, pl.ds(top, total)] = old[...]

            @pl.when(d % 2 == 0)
            def _(k=k):
                buf[2, pl.ds(top, half)] = a[k].astype(F32)

            @pl.when(d % 2 == 1)
            def _(k=k):
                buf[2, pl.ds(top, half)] = p[k].astype(F32)

            def part(j, i):
                lane = lax.broadcasted_iota(jnp.int32, (32, lanes), 1)
                at = offsets[j] // lanes + i * 32
                r = offsets[j] % lanes
                back = (lanes - r) % lanes
                here = pltpu.roll(buf[j, pl.ds(at, 32)], back, 1)
                then = pltpu.roll(buf[j, pl.ds(at + 1, 32)], back, 1)
                return jnp.where(lane < lanes - r, here, then)

            for low in (True, False):

                @pl.loop(0, half // 32)
                def _(step, k=k, out=out, low=low):
                    i = step if low else step + half // 32
                    lane = lax.broadcasted_iota(jnp.int32, (32, lanes), 1)
                    row = lax.broadcasted_iota(jnp.int32, (32, lanes), 0)
                    position = start + i * (32 * lanes) + row * lanes + lane
                    if low:
                        value = jnp.where(position < first, part(0, i), part(1, i))
                    else:
                        value = jnp.where(position >= end, part(2, i), part(1, i))
                    at = pl.ds(i * 32, 32)
                    out[at] = value
                    state[2 + k, at] = value.astype(BF)

        high = w[...].astype(BF)
        state[0] = high
        state[1] = (w[...] - high.astype(F32)).astype(BF)

    size = rows * lanes
    outs = [pltpu.VMEM((rows, lanes), F32)] * 2 + [pltpu.VMEM((4, rows, lanes), BF)]
    return call(
        body,
        where,
        (m_old, v_old, before, after, passed, master),
        outs,
        [pltpu.VMEM((3, reach, lanes), F32)],
        40 * size,
        40 * size,
    )


def step(grads, master, m_old, v_old, old_bounds):
    count = 128
    width = master.shape[0]
    rows = width // 128
    device = lax.axis_index(DP)
    z, y, x, c = coords(device)
    mine = [table(c, z, y, x, s) for s in range(4)]
    theirs = [table(1 - c, z, y, x, s) for s in range(4)]
    g = grads[0].reshape(128, rows, 128)

    given, kept, swapped = {}, {}, {}
    (given[2],) = fetch(g, (theirs[2], BF))
    swapped[2] = send(given[2], "core")
    kept[2], given[1], given[3] = fetch(g, (mine[2], F32), (theirs[1], BF), (theirs[3], BF))
    swapped[1] = send(given[1], "core")
    swapped[3] = send(given[3], "core")
    kept[1], kept[3] = fetch(g, (mine[1], F32), (mine[3], F32))
    given[0], kept[0] = fetch(g, (theirs[0], BF), (mine[0], F32))
    swapped[0] = send(given[0], "core")
    low, high = (0, 8), (8, 8)

    def local_sum(s, half, *more):
        (value,) = sum_piece([[(kept[s], *half)], [(swapped[s], *half)]] + [[(v, 0, 8)] for v in more], [(8, BF)])
        return value

    two_low, two_high = sum_piece([[(kept[2], 0, 16)], [(swapped[2], 0, 16)]], [(8, BF)] * 2)
    passing_low = send(two_low, "a", 1)
    passing_high = send(two_high, "a", 3)
    left_high = send(local_sum(1, high), "a", 1)
    right_low = send(local_sum(3, low), "a", 3)
    joined_low = local_sum(1, low, passing_low)
    left_low = send(joined_low, "a", 1)
    joined_high = local_sum(3, high, passing_high)
    right_high = send(joined_high, "a", 3)
    master_tiles = master.reshape(rows, 128)
    m_tiles, v_tiles = m_old[0].reshape(-1, 128), v_old[0].reshape(-1, 128)
    where = jnp.concatenate([old_bounds, device[None].astype(jnp.int32)])
    up, down = packed_moments(where, m_tiles, v_tiles, rows // 2)
    before = lax.ppermute(up, DP, [(d, d + 1) for d in range(127)])
    after = send(down, "core")
    passed = lax.ppermute(after, DP, [(d, d - 2) for d in range(3, 128, 2)])
    m_prev, v_prev, state = old_moments(where, m_tiles, v_tiles, before, after, passed, master_tiles)
    states = [state] + [None] * 3
    for s in (2, 1, 3):
        states[4 - s] = send(state, "z", s)
    own, q1, q2, q3 = sum_piece(
        [
            [(kept[0], 0, 16)],
            [(swapped[0], 0, 16)],
            [(left_low, 0, 8), (left_high, 0, 8)],
            [(right_low, 0, 8), (right_high, 0, 8)],
        ],
        [(4, F32)] + [(4, BF)] * 3,
    )
    q2, q1, q3 = send(q2, "b", 2), send(q1, "b", 1), send(q3, "b", 3)
    (partial,) = sum_piece([[(v, 0, 4)] for v in (own, q1, q2, q3)], [(4, BF)])
    w2, w1, w3 = send(partial, "z", 2), send(partial, "z", 1), send(partial, "z", 3)
    gradient, squares = total_piece(partial, w1, w2, w3, 32)
    squares = lax.all_to_all(squares, ("y", "x", "core"), 0, 0, tiled=True)
    piece, clip = updated_piece(gradient, states, squares, count * width)
    new = adam(master_tiles, m_prev, v_prev, gradient[0], clip[0, 0])
    master_new, m_new, v_new = (value.reshape(width) for value in new)

    got = {}
    for s in (3, 2, 1):
        got[s] = send(piece, "b", s)
    halves = {}
    halves[0, 0] = joined(piece, got[3])
    halves[0, 1] = joined(got[2], got[1])
    for h in range(2):
        halves[3, h] = send(halves[0, h], "a", 1)
        halves[1, h] = send(halves[0, h], "a", 3)
    halves[2, 0] = send(halves[3, 0], "a", 1)
    halves[2, 1] = send(halves[1, 1], "a", 3)
    partner = {}
    for r, h in halves:
        partner[r, h] = send(halves[r, h], "core")
    out = None
    for keys in (((0, 0), (0, 1)), ((3, 0), (1, 0)), ((3, 1), (1, 1)), ((2, 0), (2, 1))):
        for tables, values in ((mine, halves), (theirs, partner)):
            out = place([(tables[r][8 * h : 8 * h + 8], values[r, h]) for r, h in keys], out)
    return (master_new, m_new, v_new, out.reshape(count * width))


def solution(mesh):
    finer = Mesh(mesh.devices.reshape(4, 4, 4, 2), DP)
    placed = (P(DP, None), P(DP), P(DP, None), P(DP, None), P())
    return jax.shard_map(step, mesh=finer, in_specs=placed, out_specs=(P(DP), P(DP), P(DP), P()), check_vma=False)
```

```python
import jax
import jax.numpy as jnp
from jax import lax
from jax.experimental import pallas as pl
from jax.experimental.pallas import tpu as pltpu
from jax.sharding import Mesh
from jax.sharding import PartitionSpec as P

DP = ("z", "y", "x", "core")
BF = jnp.bfloat16
F32 = jnp.float32


def coords(d):
    return d // 32, d // 8 % 4, d // 2 % 4, d % 2


def shard_of(z, y, x, c):
    return ((z * 4 + y) * 4 + x) * 2 + c


def perm(axis, s):
    pairs = []
    for d in range(128):
        z, y, x, c = coords(d)
        if axis == "core":
            c = 1 - c
        elif axis == "z":
            z = (z + s) % 4
        elif (axis == "a") == (c == 0):
            x = (x + s) % 4
        else:
            y = (y + s) % 4
        pairs.append((d, shard_of(z, y, x, c)))
    return pairs


def send(value, axis, s=1):
    return lax.ppermute(value, DP, perm(axis, s))


def table(z, y, x, core):
    i = jnp.arange(128, dtype=jnp.int32)
    c = (core + i // 64) % 2
    s, rb, rz = i // 16 % 4, i // 4 % 4, i % 4
    zz = (z + rz) % 4
    on_0 = shard_of(zz, (y + rb) % 4, (x + s) % 4, 0)
    on_1 = shard_of(zz, (y + s) % 4, (x + rb) % 4, 1)
    return jnp.where(c == 0, on_0, on_1).astype(jnp.int32)


def cost(flops, nbytes):
    return pl.CostEstimate(flops=flops, transcendentals=0, bytes_accessed=nbytes)


def call(body, t, operands, outs, scratch, flops, nbytes, aliases=None, spaces=None, limit=8):
    vmem = pl.BlockSpec(memory_space=pltpu.VMEM)
    hbm = pl.BlockSpec(memory_space=pltpu.HBM)
    spaces = spaces or [True] * len(operands)
    operands = [pltpu.with_memory_space_constraint(o, pltpu.VMEM if v else pltpu.HBM) for o, v in zip(operands, spaces)]
    return pl.pallas_call(
        body,
        grid_spec=pltpu.PrefetchScalarGridSpec(
            num_scalar_prefetch=1,
            grid=(1,),
            in_specs=[vmem if v else hbm for v in spaces],
            out_specs=[hbm if isinstance(o, jax.ShapeDtypeStruct) else vmem for o in outs],
            scratch_shapes=scratch,
        ),
        out_shape=outs,
        input_output_aliases=aliases or {},
        cost_estimate=cost(flops, nbytes),
        compiler_params=pltpu.CompilerParams(vmem_limit_bytes=limit * 2**20),
    )(t, *operands)


def fetch(t, g, *pieces):
    _, rows, lanes = g.shape
    n = 16
    kept = [dtype == g.dtype for _, dtype in pieces]
    m = len(pieces)

    def body(t_ref, g_ref, *refs):
        outs, rest = refs[:m], refs[m:]
        sem, buf = rest[-1], rest[0]
        copies = []
        for k in range(m):
            slot = sum(not v for v in kept[:k]) * n
            for i in range(n):
                to = outs[k].at[i] if kept[k] else buf.at[slot + i]
                copies.append((k, i, slot + i, pltpu.make_async_copy(g_ref.at[t_ref[pieces[k][0] + i]], to, sem.at[k * n + i])))
        for *_, copy in copies:
            copy.start()
        for k, i, at, copy in copies:
            copy.wait()
            if not kept[k]:
                outs[k][i] = buf[at].astype(outs[k].dtype)

    converted = m - sum(kept)
    scratch = [pltpu.VMEM((converted * n, rows, lanes), g.dtype)] if converted else []
    size = m * n * rows * lanes
    return call(
        body,
        t,
        (g,),
        [pltpu.VMEM((n, rows, lanes), dtype) for _, dtype in pieces],
        scratch + [pltpu.SemaphoreType.DMA((m * n,))],
        size,
        6 * size,
        spaces=[False],
        limit=2 + 2 * converted,
    )


def sum_piece(parts, kinds):
    rows, lanes = parts[0][0][0].shape[1:]
    operands = [array for part in parts for array, _, _ in part]

    def sources(base):
        at = 0
        for part in parts:
            begin = 0
            for k, (_, first, count) in enumerate(part):
                if begin <= base < begin + count:
                    yield at + k, first + base - begin
                begin += count
            at += len(part)

    def body(t_ref, *refs):
        ins, outs = refs[: len(operands)], refs[len(operands) :]
        base = 0
        for o, (count, _) in zip(outs, kinds):
            where = list(sources(base))

            @pl.loop(0, count)
            def _(i, o=o, where=where):
                value = None
                for k, first in where:
                    term = ins[k][first + i].astype(F32)
                    value = term if value is None else value + term
                o[i] = value.astype(o.dtype)

            base += count

    size = sum(count for count, _ in kinds) * rows * lanes
    outs = [pltpu.VMEM((count, rows, lanes), dtype) for count, dtype in kinds]
    return call(body, jnp.zeros((1,), jnp.int32), operands, outs, [], len(parts) * size, (4 + 2 * len(parts)) * size)


def joined(first, second):
    def body(t_ref, a, b, o):
        o[: a.shape[0]] = a[...]
        o[a.shape[0] :] = b[...]

    shape = (first.shape[0] + second.shape[0], *first.shape[1:])
    n = first.size + second.size
    outs = [pltpu.VMEM(shape, first.dtype)]
    return call(body, jnp.zeros((1,), jnp.int32), (first, second), outs, [], n, 4 * n)[0]


def place(t, pairs, out):
    k = len(pairs)
    rows, lanes = pairs[0][1].shape[1:]
    counts = [piece.shape[0] for _, piece in pairs]

    def body(t_ref, *refs):
        o, sem = refs[-2:]
        copies = []
        for j, (first, _) in enumerate(pairs):
            for i in range(counts[j]):
                copies.append(pltpu.make_async_copy(refs[j].at[i], o.at[t_ref[first + i]], sem.at[len(copies)]))
        for copy in copies:
            copy.start()
        for copy in copies:
            copy.wait()

    operands = [piece for _, piece in pairs] + ([] if out is None else [out])
    nbytes = 4 * sum(counts) * rows * lanes
    return call(
        body,
        t,
        operands,
        [jax.ShapeDtypeStruct((128, rows, lanes), BF)],
        [pltpu.SemaphoreType.DMA((sum(counts),))],
        nbytes,
        nbytes,
        {} if out is None else {k + 1: 0},
        [True] * k + [False] * (0 if out is None else 1),
    )[0]


def total_piece(own, from1, from2, from3, copies):
    n, rows, lanes = own.shape

    def body(t_ref, w, x1, x2, x3, g, squares):
        sums = []
        for r in range(n):

            def step(i, acc, r=r):
                at = pl.ds(i * 16, 16)
                even = w[r, at].astype(F32) + x2[(r + 2) % n, at].astype(F32)
                odd = x1[(r + 1) % n, at].astype(F32) + x3[(r + 3) % n, at].astype(F32)
                value = even + odd
                g[r, at] = value
                return acc + value * value

            sums.append(lax.fori_loop(0, rows // 16, step, jnp.zeros((16, lanes), F32)))
        acc = (sums[0] + sums[2]) + (sums[1] + sums[3])
        squares[...] = jnp.broadcast_to(jnp.sum(acc), squares.shape)

    size = n * rows * lanes
    outs = [pltpu.VMEM((n, rows, lanes), F32), pltpu.VMEM((copies, 8, lanes), F32)]
    return call(body, jnp.zeros((1,), jnp.int32), (own, from1, from2, from3), outs, [], 6 * size, 12 * size)


def adam(master, m_prev, v_prev, gradient, clip):
    clipped = clip * gradient
    m_new = 0.5 * m_prev + 0.5 * clipped
    v_new = 0.95 * v_prev + 0.05 * clipped * clipped
    direction = m_new / (1.0 - 0.5**20) / (jnp.sqrt(v_new / (1.0 - 0.95**20)) + 1e-08)
    return master - 0.05 * (direction + 0.1 * master), m_new, v_new


def updated_piece(gradient, states, squares, flat):
    n, rows, lanes = gradient.shape

    def body(t_ref, g, *refs):
        state, part, piece, clip_ref = refs[:n], refs[n], refs[n + 1], refs[n + 2]
        total = part[0]
        for i in range(1, part.shape[0]):
            total = total + part[i]
        clip = jnp.minimum(1.0, jnp.sqrt(jnp.float32(flat)) / (jnp.sqrt(total) + 1e-06))
        clip_ref[...] = clip
        clip = jnp.concatenate([clip, clip])
        for r in range(n):

            @pl.loop(0, rows // 16)
            def _(i, r=r):
                at = pl.ds(i * 16, 16)
                high, low, m, v = (state[r][k, at].astype(F32) for k in range(4))
                piece[r, at] = adam(high + low, m, v, g[r, at], clip)[0].astype(BF)

    size = n * rows * lanes
    outs = [pltpu.VMEM((n, rows, lanes), BF), pltpu.VMEM((8, lanes), F32)]
    return call(body, jnp.zeros((1,), jnp.int32), (gradient, *states, squares), outs, [], 20 * size, 14 * size)


def moved_rows(end, half, lanes, total):
    return jnp.minimum(jnp.maximum(end - half * lanes, 0) // lanes, total - half - 8)


def packed_moments(where, m_old, v_old, half):
    total, lanes = m_old.shape
    last = where.shape[0] - 1

    def body(t_ref, m, v, up, down):
        d = t_ref[last]
        q = moved_rows(t_ref[d + 1] - t_ref[d], half, lanes, total)
        for k, old in enumerate((m, v)):
            up[k] = old[pl.ds(q, half + 8)].astype(BF)
            down[k] = old[pl.ds(0, half)].astype(BF)

    n = 4 * half * lanes
    outs = [pltpu.VMEM((2, half + 8, lanes), BF), pltpu.VMEM((2, half, lanes), BF)]
    return call(body, where, (m_old, v_old), outs, [], n, 6 * n)


def old_moments(where, m_old, v_old, before, after, passed, master):
    rows, lanes = master.shape
    total = m_old.shape[0]
    half = rows // 2
    top = 392
    reach = top + total + half + 8
    last = where.shape[0] - 1

    def body(t_ref, m, v, b, a, p, w, m_out, v_out, state, buf):
        d = t_ref[last]
        start = d * (rows * lanes)
        first = t_ref[d]
        end = t_ref[d + 1]
        ahead = t_ref[jnp.maximum(d - 1, 0)]
        q = moved_rows(first - ahead, half, lanes, total)
        offsets = [start - s + top * lanes for s in (ahead + q * lanes, first, end)]
        for k, (old, out) in enumerate(((m, m_out), (v, v_out))):
            buf[0, pl.ds(top, half + 8)] = b[k].astype(F32)
            buf[1, pl.ds(top, total)] = old[...]

            @pl.when(d % 2 == 0)
            def _(k=k):
                buf[2, pl.ds(top, half)] = a[k].astype(F32)

            @pl.when(d % 2 == 1)
            def _(k=k):
                buf[2, pl.ds(top, half)] = p[k].astype(F32)

            def part(j, i):
                lane = lax.broadcasted_iota(jnp.int32, (32, lanes), 1)
                at = offsets[j] // lanes + i * 32
                r = offsets[j] % lanes
                back = (lanes - r) % lanes
                here = pltpu.roll(buf[j, pl.ds(at, 32)], back, 1)
                then = pltpu.roll(buf[j, pl.ds(at + 1, 32)], back, 1)
                return jnp.where(lane < lanes - r, here, then)

            for low in (True, False):

                @pl.loop(0, half // 32)
                def _(step, k=k, out=out, low=low):
                    i = step if low else step + half // 32
                    lane = lax.broadcasted_iota(jnp.int32, (32, lanes), 1)
                    row = lax.broadcasted_iota(jnp.int32, (32, lanes), 0)
                    position = start + i * (32 * lanes) + row * lanes + lane
                    if low:
                        value = jnp.where(position < first, part(0, i), part(1, i))
                    else:
                        value = jnp.where(position >= end, part(2, i), part(1, i))
                    at = pl.ds(i * 32, 32)
                    out[at] = value
                    state[2 + k, at] = value.astype(BF)

        high = w[...].astype(BF)
        state[0] = high
        state[1] = (w[...] - high.astype(F32)).astype(BF)

    size = rows * lanes
    outs = [pltpu.VMEM((rows, lanes), F32)] * 2 + [pltpu.VMEM((4, rows, lanes), BF)]
    return call(
        body,
        where,
        (m_old, v_old, before, after, passed, master),
        outs,
        [pltpu.VMEM((3, reach, lanes), F32)],
        40 * size,
        40 * size,
    )


def step(grads, master, m_old, v_old, old_bounds):
    count = 128
    width = master.shape[0]
    rows = width // 128
    device = lax.axis_index(DP)
    z, y, x, c = coords(device)
    places = table(z, y, x, c)
    mine = [16 * s for s in range(4)]
    theirs = [64 + 16 * s for s in range(4)]
    g = grads[0].reshape(128, rows, 128)

    given, kept, swapped = {}, {}, {}
    (given[2],) = fetch(places, g, (theirs[2], BF))
    swapped[2] = send(given[2], "core")
    kept[2], given[1], given[3] = fetch(places, g, (mine[2], F32), (theirs[1], BF), (theirs[3], BF))
    swapped[1] = send(given[1], "core")
    swapped[3] = send(given[3], "core")
    kept[1], kept[3] = fetch(places, g, (mine[1], F32), (mine[3], F32))
    given[0], kept[0] = fetch(places, g, (theirs[0], BF), (mine[0], F32))
    swapped[0] = send(given[0], "core")
    low, high = (0, 8), (8, 8)

    def local_sum(s, half, *more):
        (value,) = sum_piece([[(kept[s], *half)], [(swapped[s], *half)]] + [[(v, 0, 8)] for v in more], [(8, BF)])
        return value

    two_low, two_high = sum_piece([[(kept[2], 0, 16)], [(swapped[2], 0, 16)]], [(8, BF)] * 2)
    passing_low = send(two_low, "a", 1)
    passing_high = send(two_high, "a", 3)
    left_high = send(local_sum(1, high), "a", 1)
    right_low = send(local_sum(3, low), "a", 3)
    joined_low = local_sum(1, low, passing_low)
    left_low = send(joined_low, "a", 1)
    joined_high = local_sum(3, high, passing_high)
    right_high = send(joined_high, "a", 3)
    master_tiles = master.reshape(rows, 128)
    m_tiles, v_tiles = m_old[0].reshape(-1, 128), v_old[0].reshape(-1, 128)
    where = jnp.concatenate([old_bounds, device[None].astype(jnp.int32)])
    up, down = packed_moments(where, m_tiles, v_tiles, rows // 2)
    before = lax.ppermute(up, DP, [(d, d + 1) for d in range(127)])
    after = send(down, "core")
    passed = lax.ppermute(after, DP, [(d, d - 2) for d in range(3, 128, 2)])
    m_prev, v_prev, state = old_moments(where, m_tiles, v_tiles, before, after, passed, master_tiles)
    states = [state] + [None] * 3
    for s in (2, 1, 3):
        states[4 - s] = send(state, "z", s)
    own, q1, q2, q3 = sum_piece(
        [
            [(kept[0], 0, 16)],
            [(swapped[0], 0, 16)],
            [(left_low, 0, 8), (left_high, 0, 8)],
            [(right_low, 0, 8), (right_high, 0, 8)],
        ],
        [(4, F32)] + [(4, BF)] * 3,
    )
    quarters = {2: q2, 1: q1, 3: q3}
    for s in (2, 1, 3):
        quarters[s] = send(quarters[s], "b", s)
    (partial,) = sum_piece([[(v, 0, 4)] for v in (own, quarters[1], quarters[2], quarters[3])], [(4, BF)])
    w2, w1, w3 = send(partial, "z", 2), send(partial, "z", 1), send(partial, "z", 3)
    gradient, squares = total_piece(partial, w1, w2, w3, 32)
    squares = lax.all_to_all(squares, ("y", "x", "core"), 0, 0, tiled=True)
    piece, clip = updated_piece(gradient, states, squares, count * width)
    new = adam(master_tiles, m_prev, v_prev, gradient[0], clip[0, 0])
    master_new, m_new, v_new = (value.reshape(width) for value in new)

    got = {}
    for s in (3, 2, 1):
        got[s] = send(piece, "b", s)
    halves = {}
    halves[0, 0] = joined(piece, got[3])
    halves[0, 1] = joined(got[2], got[1])
    for h in range(2):
        halves[3, h] = send(halves[0, h], "a", 1)
        halves[1, h] = send(halves[0, h], "a", 3)
    halves[2, 0] = send(halves[3, 0], "a", 1)
    halves[2, 1] = send(halves[1, 1], "a", 3)
    partner = {}
    for r, h in halves:
        partner[r, h] = send(halves[r, h], "core")
    out = None
    for keys in (((0, 0), (0, 1)), ((3, 0), (1, 0), (3, 1), (1, 1)), ((2, 0),), ((2, 1),)):
        pairs = [(mine[r] + 8 * h, halves[r, h]) for r, h in keys]
        pairs += [(theirs[r] + 8 * h, partner[r, h]) for r, h in keys]
        out = place(places, pairs, out)
    return (master_new, m_new, v_new, out.reshape(count * width))


def solution(mesh):
    finer = Mesh(mesh.devices.reshape(4, 4, 4, 2), DP)
    placed = (P(DP, None), P(DP), P(DP, None), P(DP, None), P())
    return jax.shard_map(step, mesh=finer, in_specs=placed, out_specs=(P(DP), P(DP), P(DP), P()), check_vma=False)
```

```python
import jax
import jax.numpy as jnp
from jax import lax
from jax.experimental import pallas as pl
from jax.experimental.pallas import tpu as pltpu
from jax.sharding import Mesh
from jax.sharding import PartitionSpec as P

DP = ("z", "y", "x", "core")
BF = jnp.bfloat16
F32 = jnp.float32


def coords(d):
    return d // 32, d // 8 % 4, d // 2 % 4, d % 2


def shard_of(z, y, x, c):
    return ((z * 4 + y) * 4 + x) * 2 + c


def perm(axis, s):
    pairs = []
    for d in range(128):
        z, y, x, c = coords(d)
        if axis == "core":
            c = 1 - c
        elif axis == "z":
            z = (z + s) % 4
        elif (axis == "a") == (c == 0):
            x = (x + s) % 4
        else:
            y = (y + s) % 4
        pairs.append((d, shard_of(z, y, x, c)))
    return pairs


def send(value, axis, s=1):
    return lax.ppermute(value, DP, perm(axis, s))


def table(z, y, x, core):
    i = jnp.arange(128, dtype=jnp.int32)
    c = (core + i // 64) % 2
    s, rb, rz = i // 16 % 4, i // 4 % 4, i % 4
    zz = (z + rz) % 4
    on_0 = shard_of(zz, (y + rb) % 4, (x + s) % 4, 0)
    on_1 = shard_of(zz, (y + s) % 4, (x + rb) % 4, 1)
    return jnp.where(c == 0, on_0, on_1).astype(jnp.int32)


def cost(flops, nbytes):
    return pl.CostEstimate(flops=flops, transcendentals=0, bytes_accessed=nbytes)


def call(body, t, operands, outs, scratch, flops, nbytes, aliases=None, spaces=None, limit=8):
    vmem = pl.BlockSpec(memory_space=pltpu.VMEM)
    hbm = pl.BlockSpec(memory_space=pltpu.HBM)
    spaces = spaces or [True] * len(operands)
    operands = [pltpu.with_memory_space_constraint(o, pltpu.VMEM if v else pltpu.HBM) for o, v in zip(operands, spaces)]
    return pl.pallas_call(
        body,
        grid_spec=pltpu.PrefetchScalarGridSpec(
            num_scalar_prefetch=1,
            grid=(1,),
            in_specs=[vmem if v else hbm for v in spaces],
            out_specs=[hbm if isinstance(o, jax.ShapeDtypeStruct) else vmem for o in outs],
            scratch_shapes=scratch,
        ),
        out_shape=outs,
        input_output_aliases=aliases or {},
        cost_estimate=cost(flops, nbytes),
        compiler_params=pltpu.CompilerParams(vmem_limit_bytes=limit * 2**20),
    )(t, *operands)


def fetch(t, g, *pieces):
    _, rows, lanes = g.shape
    n = 16
    kept = [dtype == g.dtype for _, dtype in pieces]
    m = len(pieces)

    def body(t_ref, g_ref, *refs):
        outs, rest = refs[:m], refs[m:]
        sem, buf = rest[-1], rest[0]
        copies = []
        for k in range(m):
            slot = sum(not v for v in kept[:k]) * n
            for i in range(n):
                to = outs[k].at[i] if kept[k] else buf.at[slot + i]
                copies.append((k, i, slot + i, pltpu.make_async_copy(g_ref.at[t_ref[pieces[k][0] + i]], to, sem.at[k * n + i])))
        for *_, copy in copies:
            copy.start()
        for k, i, at, copy in copies:
            copy.wait()
            if not kept[k]:
                outs[k][i] = buf[at].astype(outs[k].dtype)

    converted = m - sum(kept)
    scratch = [pltpu.VMEM((converted * n, rows, lanes), g.dtype)] if converted else []
    size = m * n * rows * lanes
    return call(
        body,
        t,
        (g,),
        [pltpu.VMEM((n, rows, lanes), dtype) for _, dtype in pieces],
        scratch + [pltpu.SemaphoreType.DMA((m * n,))],
        size,
        6 * size,
        spaces=[False],
        limit=2 + 2 * converted,
    )


def sum_piece(parts, kinds):
    rows, lanes = parts[0][0][0].shape[1:]
    operands = [array for part in parts for array, _, _ in part]

    def sources(base):
        at = 0
        for part in parts:
            begin = 0
            for k, (_, first, count) in enumerate(part):
                if begin <= base < begin + count:
                    yield at + k, first + base - begin
                begin += count
            at += len(part)

    def body(t_ref, *refs):
        ins, outs = refs[: len(operands)], refs[len(operands) :]
        base = 0
        for o, (count, _) in zip(outs, kinds):
            where = list(sources(base))

            @pl.loop(0, count)
            def _(i, o=o, where=where):
                value = None
                for k, first in where:
                    term = ins[k][first + i].astype(F32)
                    value = term if value is None else value + term
                o[i] = value.astype(o.dtype)

            base += count

    size = sum(count for count, _ in kinds) * rows * lanes
    outs = [pltpu.VMEM((count, rows, lanes), dtype) for count, dtype in kinds]
    return call(body, jnp.zeros((1,), jnp.int32), operands, outs, [], len(parts) * size, (4 + 2 * len(parts)) * size)


def joined(first, second):
    def body(t_ref, a, b, o):
        o[: a.shape[0]] = a[...]
        o[a.shape[0] :] = b[...]

    shape = (first.shape[0] + second.shape[0], *first.shape[1:])
    n = first.size + second.size
    outs = [pltpu.VMEM(shape, first.dtype)]
    return call(body, jnp.zeros((1,), jnp.int32), (first, second), outs, [], n, 4 * n)[0]


def place(t, pairs, out):
    k = len(pairs)
    rows, lanes = pairs[0][1].shape[1:]
    counts = [piece.shape[0] for _, piece in pairs]

    def body(t_ref, *refs):
        o, sem = refs[-2:]
        copies = []
        for j, (first, _) in enumerate(pairs):
            for i in range(counts[j]):
                copies.append(pltpu.make_async_copy(refs[j].at[i], o.at[t_ref[first + i]], sem.at[len(copies)]))
        for copy in copies:
            copy.start()
        for copy in copies:
            copy.wait()

    operands = [piece for _, piece in pairs] + ([] if out is None else [out])
    nbytes = 4 * sum(counts) * rows * lanes
    return call(
        body,
        t,
        operands,
        [jax.ShapeDtypeStruct((128, rows, lanes), BF)],
        [pltpu.SemaphoreType.DMA((sum(counts),))],
        nbytes,
        nbytes,
        {} if out is None else {k + 1: 0},
        [True] * k + [False] * (0 if out is None else 1),
    )[0]


def total_piece(own, from1, from2, from3, copies):
    n, rows, lanes = own.shape

    def body(t_ref, w, x1, x2, x3, g, squares):
        sums = []
        for r in range(n):

            def step(i, acc, r=r):
                at = pl.ds(i * 16, 16)
                even = w[r, at].astype(F32) + x2[(r + 2) % n, at].astype(F32)
                odd = x1[(r + 1) % n, at].astype(F32) + x3[(r + 3) % n, at].astype(F32)
                value = even + odd
                g[r, at] = value
                return acc + value * value

            sums.append(lax.fori_loop(0, rows // 16, step, jnp.zeros((16, lanes), F32)))
        acc = (sums[0] + sums[2]) + (sums[1] + sums[3])
        squares[...] = jnp.broadcast_to(jnp.sum(acc), squares.shape)

    size = n * rows * lanes
    outs = [pltpu.VMEM((n, rows, lanes), F32), pltpu.VMEM((copies, 8, lanes), F32)]
    return call(body, jnp.zeros((1,), jnp.int32), (own, from1, from2, from3), outs, [], 6 * size, 12 * size)


def adam(master, m_prev, v_prev, gradient, clip):
    clipped = clip * gradient
    m_new = 0.5 * m_prev + 0.5 * clipped
    v_new = 0.95 * v_prev + 0.05 * clipped * clipped
    direction = m_new / (1.0 - 0.5**20) / (jnp.sqrt(v_new / (1.0 - 0.95**20)) + 1e-08)
    return master - 0.05 * (direction + 0.1 * master), m_new, v_new


def updated_piece(gradient, states, squares, flat):
    n, rows, lanes = gradient.shape

    def body(t_ref, g, *refs):
        state, part, piece, clip_ref = refs[:n], refs[n], refs[n + 1], refs[n + 2]
        total = part[0]
        for i in range(1, part.shape[0]):
            total = total + part[i]
        clip = jnp.minimum(1.0, jnp.sqrt(jnp.float32(flat)) / (jnp.sqrt(total) + 1e-06))
        clip_ref[...] = clip
        clip = jnp.concatenate([clip, clip])
        for r in range(n):

            @pl.loop(0, rows // 16)
            def _(i, r=r):
                at = pl.ds(i * 16, 16)
                high, low, m, v = (state[r][k, at].astype(F32) for k in range(4))
                piece[r, at] = adam(high + low, m, v, g[r, at], clip)[0].astype(BF)

    size = n * rows * lanes
    outs = [pltpu.VMEM((n, rows, lanes), BF), pltpu.VMEM((8, lanes), F32)]
    return call(body, jnp.zeros((1,), jnp.int32), (gradient, *states, squares), outs, [], 20 * size, 14 * size)


def moved_rows(end, half, lanes, total):
    return jnp.minimum(jnp.maximum(end - half * lanes, 0) // lanes, total - half - 8)


def packed_moments(where, m_old, v_old, half):
    total, lanes = m_old.shape
    last = where.shape[0] - 1

    def body(t_ref, m, v, up, down):
        d = t_ref[last]
        q = moved_rows(t_ref[d + 1] - t_ref[d], half, lanes, total)
        for k, old in enumerate((m, v)):
            up[k] = old[pl.ds(q, half + 8)].astype(BF)
            down[k] = old[pl.ds(0, half)].astype(BF)

    n = 4 * half * lanes
    outs = [pltpu.VMEM((2, half + 8, lanes), BF), pltpu.VMEM((2, half, lanes), BF)]
    return call(body, where, (m_old, v_old), outs, [], n, 6 * n)


def old_moments(where, m_old, v_old, before, after, passed, master):
    rows, lanes = master.shape
    total = m_old.shape[0]
    half = rows // 2
    top = 392
    reach = top + total + half + 8
    last = where.shape[0] - 1

    def body(t_ref, m, v, b, a, p, w, m_out, v_out, state, buf):
        d = t_ref[last]
        start = d * (rows * lanes)
        first = t_ref[d]
        end = t_ref[d + 1]
        ahead = t_ref[jnp.maximum(d - 1, 0)]
        q = moved_rows(first - ahead, half, lanes, total)
        offsets = [start - s + top * lanes for s in (ahead + q * lanes, first, end)]
        for k, (old, out) in enumerate(((m, m_out), (v, v_out))):
            buf[0, pl.ds(top, half + 8)] = b[k].astype(F32)
            buf[1, pl.ds(top, total)] = old[...]

            @pl.when(d % 2 == 0)
            def _(k=k):
                buf[2, pl.ds(top, half)] = a[k].astype(F32)

            @pl.when(d % 2 == 1)
            def _(k=k):
                buf[2, pl.ds(top, half)] = p[k].astype(F32)

            def part(j, i):
                lane = lax.broadcasted_iota(jnp.int32, (32, lanes), 1)
                at = offsets[j] // lanes + i * 32
                r = offsets[j] % lanes
                back = (lanes - r) % lanes
                here = pltpu.roll(buf[j, pl.ds(at, 32)], back, 1)
                then = pltpu.roll(buf[j, pl.ds(at + 1, 32)], back, 1)
                return jnp.where(lane < lanes - r, here, then)

            for low in (True, False):

                @pl.loop(0, half // 32)
                def _(step, k=k, out=out, low=low):
                    i = step if low else step + half // 32
                    lane = lax.broadcasted_iota(jnp.int32, (32, lanes), 1)
                    row = lax.broadcasted_iota(jnp.int32, (32, lanes), 0)
                    position = start + i * (32 * lanes) + row * lanes + lane
                    if low:
                        value = jnp.where(position < first, part(0, i), part(1, i))
                    else:
                        value = jnp.where(position >= end, part(2, i), part(1, i))
                    at = pl.ds(i * 32, 32)
                    out[at] = value
                    state[2 + k, at] = value.astype(BF)

        high = w[...].astype(BF)
        state[0] = high
        state[1] = (w[...] - high.astype(F32)).astype(BF)

    size = rows * lanes
    outs = [pltpu.VMEM((rows, lanes), F32)] * 2 + [pltpu.VMEM((4, rows, lanes), BF)]
    return call(
        body,
        where,
        (m_old, v_old, before, after, passed, master),
        outs,
        [pltpu.VMEM((3, reach, lanes), F32)],
        40 * size,
        40 * size,
    )


def step(grads, master, m_old, v_old, old_bounds):
    count = 128
    width = master.shape[0]
    rows = width // 128
    device = lax.axis_index(DP)
    z, y, x, c = coords(device)
    places = table(z, y, x, c)
    mine = [16 * s for s in range(4)]
    theirs = [64 + 16 * s for s in range(4)]
    g = grads[0].reshape(128, rows, 128)

    given, kept, swapped = {}, {}, {}
    (given[2],) = fetch(places, g, (theirs[2], BF))
    swapped[2] = send(given[2], "core")
    kept[2], given[1] = fetch(places, g, (mine[2], F32), (theirs[1], BF))
    swapped[1] = send(given[1], "core")
    given[3], kept[1], kept[3] = fetch(places, g, (theirs[3], BF), (mine[1], F32), (mine[3], F32))
    swapped[3] = send(given[3], "core")
    given[0], kept[0] = fetch(places, g, (theirs[0], BF), (mine[0], F32))
    swapped[0] = send(given[0], "core")
    low, high = (0, 8), (8, 8)

    def local_sum(s, half, *more):
        (value,) = sum_piece([[(kept[s], *half)], [(swapped[s], *half)]] + [[(v, 0, 8)] for v in more], [(8, BF)])
        return value

    two_low, two_high = sum_piece([[(kept[2], 0, 16)], [(swapped[2], 0, 16)]], [(8, BF)] * 2)
    passing_low = send(two_low, "a", 1)
    passing_high = send(two_high, "a", 3)
    left_high = send(local_sum(1, high), "a", 1)
    right_low = send(local_sum(3, low), "a", 3)
    joined_low = local_sum(1, low, passing_low)
    left_low = send(joined_low, "a", 1)
    joined_high = local_sum(3, high, passing_high)
    right_high = send(joined_high, "a", 3)
    master_tiles = master.reshape(rows, 128)
    m_tiles, v_tiles = m_old[0].reshape(-1, 128), v_old[0].reshape(-1, 128)
    where = jnp.concatenate([old_bounds, device[None].astype(jnp.int32)])
    up, down = packed_moments(where, m_tiles, v_tiles, rows // 2)
    before = lax.ppermute(up, DP, [(d, d + 1) for d in range(127)])
    after = send(down, "core")
    passed = lax.ppermute(after, DP, [(d, d - 2) for d in range(3, 128, 2)])
    m_prev, v_prev, state = old_moments(where, m_tiles, v_tiles, before, after, passed, master_tiles)
    states = [state] + [None] * 3
    for s in (2, 1, 3):
        states[4 - s] = send(state, "z", s)
    own, q1, q2, q3 = sum_piece(
        [
            [(kept[0], 0, 16)],
            [(swapped[0], 0, 16)],
            [(left_low, 0, 8), (left_high, 0, 8)],
            [(right_low, 0, 8), (right_high, 0, 8)],
        ],
        [(4, F32)] + [(4, BF)] * 3,
    )
    quarters = {2: q2, 1: q1, 3: q3}
    for s in (2, 1, 3):
        quarters[s] = send(quarters[s], "b", s)
    (partial,) = sum_piece([[(v, 0, 4)] for v in (own, quarters[1], quarters[2], quarters[3])], [(4, BF)])
    parts = {}
    for s in (2, 1, 3):
        parts[s] = send(partial, "z", s)
    gradient, squares = total_piece(partial, parts[1], parts[2], parts[3], 32)
    squares = lax.all_to_all(squares, ("y", "x", "core"), 0, 0, tiled=True)
    piece, clip = updated_piece(gradient, states, squares, count * width)
    new = adam(master_tiles, m_prev, v_prev, gradient[0], clip[0, 0])
    master_new, m_new, v_new = (value.reshape(width) for value in new)

    got = {}
    for s in (3, 2, 1):
        got[s] = send(piece, "b", s)
    halves = {}
    halves[0, 0] = joined(piece, got[3])
    halves[0, 1] = joined(got[2], got[1])
    for h in range(2):
        halves[3, h] = send(halves[0, h], "a", 1)
        halves[1, h] = send(halves[0, h], "a", 3)
    halves[2, 0] = send(halves[3, 0], "a", 1)
    halves[2, 1] = send(halves[1, 1], "a", 3)
    partner = {}
    for r, h in halves:
        partner[r, h] = send(halves[r, h], "core")
    out = None
    for keys in (((0, 0), (0, 1)), ((3, 0), (1, 0), (3, 1), (1, 1), (2, 0)), ((2, 1),)):
        pairs = [(mine[r] + 8 * h, halves[r, h]) for r, h in keys]
        pairs += [(theirs[r] + 8 * h, partner[r, h]) for r, h in keys]
        out = place(places, pairs, out)
    return (master_new, m_new, v_new, out.reshape(count * width))


def solution(mesh):
    finer = Mesh(mesh.devices.reshape(4, 4, 4, 2), DP)
    placed = (P(DP, None), P(DP), P(DP, None), P(DP, None), P())
    return jax.shard_map(step, mesh=finer, in_specs=placed, out_specs=(P(DP), P(DP), P(DP), P()), check_vma=False)
```

```python
import jax
import jax.numpy as jnp
from jax import lax
from jax.experimental import pallas as pl
from jax.experimental.pallas import tpu as pltpu
from jax.sharding import Mesh
from jax.sharding import PartitionSpec as P

DP = ("z", "y", "x", "core")
BF = jnp.bfloat16
F32 = jnp.float32


def coords(d):
    return d // 32, d // 8 % 4, d // 2 % 4, d % 2


def shard_of(z, y, x, c):
    return ((z * 4 + y) * 4 + x) * 2 + c


def perm(axis, s):
    pairs = []
    for d in range(128):
        z, y, x, c = coords(d)
        if axis == "core":
            c = 1 - c
        elif axis == "z":
            z = (z + s) % 4
        elif (axis == "a") == (c == 0):
            x = (x + s) % 4
        else:
            y = (y + s) % 4
        pairs.append((d, shard_of(z, y, x, c)))
    return pairs


def send(value, axis, s=1):
    return lax.ppermute(value, DP, perm(axis, s))


def table(z, y, x, core):
    i = jnp.arange(128, dtype=jnp.int32)
    c = (core + i // 64) % 2
    s, rb, rz = i // 16 % 4, i // 4 % 4, i % 4
    zz = (z + rz) % 4
    on_0 = shard_of(zz, (y + rb) % 4, (x + s) % 4, 0)
    on_1 = shard_of(zz, (y + s) % 4, (x + rb) % 4, 1)
    return jnp.where(c == 0, on_0, on_1).astype(jnp.int32)


def cost(flops, nbytes):
    return pl.CostEstimate(flops=flops, transcendentals=0, bytes_accessed=nbytes)


def call(body, t, operands, outs, scratch, flops, nbytes, aliases=None, spaces=None, limit=8):
    vmem = pl.BlockSpec(memory_space=pltpu.VMEM)
    hbm = pl.BlockSpec(memory_space=pltpu.HBM)
    spaces = spaces or [True] * len(operands)
    operands = [pltpu.with_memory_space_constraint(o, pltpu.VMEM if v else pltpu.HBM) for o, v in zip(operands, spaces)]
    return pl.pallas_call(
        body,
        grid_spec=pltpu.PrefetchScalarGridSpec(
            num_scalar_prefetch=1,
            grid=(1,),
            in_specs=[vmem if v else hbm for v in spaces],
            out_specs=[hbm if isinstance(o, jax.ShapeDtypeStruct) else vmem for o in outs],
            scratch_shapes=scratch,
        ),
        out_shape=outs,
        input_output_aliases=aliases or {},
        cost_estimate=cost(flops, nbytes),
        compiler_params=pltpu.CompilerParams(vmem_limit_bytes=limit * 2**20),
    )(t, *operands)


def fetch(t, g, *pieces):
    _, rows, lanes = g.shape
    n = 16
    kept = [dtype == g.dtype for _, dtype in pieces]
    m = len(pieces)

    def body(t_ref, g_ref, *refs):
        outs, rest = refs[:m], refs[m:]
        sem, buf = rest[-1], rest[0]
        copies = []
        for k in range(m):
            slot = sum(not v for v in kept[:k]) * n
            for i in range(n):
                to = outs[k].at[i] if kept[k] else buf.at[slot + i]
                copies.append((k, i, slot + i, pltpu.make_async_copy(g_ref.at[t_ref[pieces[k][0] + i]], to, sem.at[k * n + i])))
        for *_, copy in copies:
            copy.start()
        for k, i, at, copy in copies:
            copy.wait()
            if not kept[k]:
                outs[k][i] = buf[at].astype(outs[k].dtype)

    converted = m - sum(kept)
    scratch = [pltpu.VMEM((converted * n, rows, lanes), g.dtype)] if converted else []
    size = m * n * rows * lanes
    return call(
        body,
        t,
        (g,),
        [pltpu.VMEM((n, rows, lanes), dtype) for _, dtype in pieces],
        scratch + [pltpu.SemaphoreType.DMA((m * n,))],
        size,
        6 * size,
        spaces=[False],
        limit=2 + 2 * converted,
    )


def sum_piece(parts, kinds):
    rows, lanes = parts[0][0][0].shape[1:]
    operands = [array for part in parts for array, _, _ in part]

    def sources(base):
        at = 0
        for part in parts:
            begin = 0
            for k, (_, first, count) in enumerate(part):
                if begin <= base < begin + count:
                    yield at + k, first + base - begin
                begin += count
            at += len(part)

    def body(t_ref, *refs):
        ins, outs = refs[: len(operands)], refs[len(operands) :]
        base = 0
        for o, (count, _) in zip(outs, kinds):
            where = list(sources(base))

            @pl.loop(0, count)
            def _(i, o=o, where=where):
                value = None
                for k, first in where:
                    term = ins[k][first + i].astype(F32)
                    value = term if value is None else value + term
                o[i] = value.astype(o.dtype)

            base += count

    size = sum(count for count, _ in kinds) * rows * lanes
    outs = [pltpu.VMEM((count, rows, lanes), dtype) for count, dtype in kinds]
    return call(body, jnp.zeros((1,), jnp.int32), operands, outs, [], len(parts) * size, (4 + 2 * len(parts)) * size)


def joined(first, second):
    def body(t_ref, a, b, o):
        o[: a.shape[0]] = a[...]
        o[a.shape[0] :] = b[...]

    shape = (first.shape[0] + second.shape[0], *first.shape[1:])
    n = first.size + second.size
    outs = [pltpu.VMEM(shape, first.dtype)]
    return call(body, jnp.zeros((1,), jnp.int32), (first, second), outs, [], n, 4 * n)[0]


def place(t, pairs, out):
    k = len(pairs)
    rows, lanes = pairs[0][1].shape[1:]
    counts = [piece.shape[0] for _, piece in pairs]

    def body(t_ref, *refs):
        o, sem = refs[-2:]
        copies = []
        for j, (first, _) in enumerate(pairs):
            for i in range(counts[j]):
                copies.append(pltpu.make_async_copy(refs[j].at[i], o.at[t_ref[first + i]], sem.at[len(copies)]))
        for copy in copies:
            copy.start()
        for copy in copies:
            copy.wait()

    operands = [piece for _, piece in pairs] + ([] if out is None else [out])
    nbytes = 4 * sum(counts) * rows * lanes
    return call(
        body,
        t,
        operands,
        [jax.ShapeDtypeStruct((128, rows, lanes), BF)],
        [pltpu.SemaphoreType.DMA((sum(counts),))],
        nbytes,
        nbytes,
        {} if out is None else {k + 1: 0},
        [True] * k + [False] * (0 if out is None else 1),
    )[0]


def total_piece(own, from1, from2, from3, copies):
    n, rows, lanes = own.shape

    def body(t_ref, w, x1, x2, x3, g, squares):
        sums = []
        for r in range(n):

            def step(i, acc, r=r):
                at = pl.ds(i * 16, 16)
                even = w[r, at].astype(F32) + x2[(r + 2) % n, at].astype(F32)
                odd = x1[(r + 1) % n, at].astype(F32) + x3[(r + 3) % n, at].astype(F32)
                value = even + odd
                g[r, at] = value
                return acc + value * value

            sums.append(lax.fori_loop(0, rows // 16, step, jnp.zeros((16, lanes), F32)))
        acc = (sums[0] + sums[2]) + (sums[1] + sums[3])
        squares[...] = jnp.broadcast_to(jnp.sum(acc), squares.shape)

    size = n * rows * lanes
    outs = [pltpu.VMEM((n, rows, lanes), F32), pltpu.VMEM((copies, 8, lanes), F32)]
    return call(body, jnp.zeros((1,), jnp.int32), (own, from1, from2, from3), outs, [], 6 * size, 12 * size)


def adam(master, m_prev, v_prev, gradient, clip):
    clipped = clip * gradient
    m_new = 0.5 * m_prev + 0.5 * clipped
    v_new = 0.95 * v_prev + 0.05 * clipped * clipped
    direction = m_new / (1.0 - 0.5**20) / (jnp.sqrt(v_new / (1.0 - 0.95**20)) + 1e-08)
    return master - 0.05 * (direction + 0.1 * master), m_new, v_new


def updated_piece(gradient, states, squares, flat):
    n, rows, lanes = gradient.shape

    def body(t_ref, g, *refs):
        state, part, piece, clip_ref = refs[:n], refs[n], refs[n + 1], refs[n + 2]
        total = part[0]
        for i in range(1, part.shape[0]):
            total = total + part[i]
        clip = jnp.minimum(1.0, jnp.sqrt(jnp.float32(flat)) / (jnp.sqrt(total) + 1e-06))
        clip_ref[...] = clip
        clip = jnp.concatenate([clip, clip])
        for r in range(n):

            @pl.loop(0, rows // 16)
            def _(i, r=r):
                at = pl.ds(i * 16, 16)
                high, low, m, v = (state[r][k, at].astype(F32) for k in range(4))
                piece[r, at] = adam(high + low, m, v, g[r, at], clip)[0].astype(BF)

    size = n * rows * lanes
    outs = [pltpu.VMEM((n, rows, lanes), BF), pltpu.VMEM((8, lanes), F32)]
    return call(body, jnp.zeros((1,), jnp.int32), (gradient, *states, squares), outs, [], 20 * size, 14 * size)


def moved_rows(end, half, lanes, total):
    return jnp.minimum(jnp.maximum(end - half * lanes, 0) // lanes, total - half - 8)


def packed_moments(where, m_old, v_old, half):
    total, lanes = m_old.shape
    last = where.shape[0] - 1

    def body(t_ref, m, v, up, down):
        d = t_ref[last]
        q = moved_rows(t_ref[d + 1] - t_ref[d], half, lanes, total)
        for k, old in enumerate((m, v)):
            up[k] = old[pl.ds(q, half + 8)].astype(BF)
            down[k] = old[pl.ds(0, half)].astype(BF)

    n = 4 * half * lanes
    outs = [pltpu.VMEM((2, half + 8, lanes), BF), pltpu.VMEM((2, half, lanes), BF)]
    return call(body, where, (m_old, v_old), outs, [], n, 6 * n)


def old_moments(where, m_old, v_old, before, after, passed, master):
    rows, lanes = master.shape
    total = m_old.shape[0]
    half = rows // 2
    top = 392
    reach = top + total + half + 8
    last = where.shape[0] - 1

    def body(t_ref, m, v, b, a, p, w, m_out, v_out, state, buf):
        d = t_ref[last]
        start = d * (rows * lanes)
        first = t_ref[d]
        end = t_ref[d + 1]
        ahead = t_ref[jnp.maximum(d - 1, 0)]
        q = moved_rows(first - ahead, half, lanes, total)
        offsets = [start - s + top * lanes for s in (ahead + q * lanes, first, end)]
        for k, (old, out) in enumerate(((m, m_out), (v, v_out))):
            buf[0, pl.ds(top, half + 8)] = b[k].astype(F32)
            buf[1, pl.ds(top, total)] = old[...]

            @pl.when(d % 2 == 0)
            def _(k=k):
                buf[2, pl.ds(top, half)] = a[k].astype(F32)

            @pl.when(d % 2 == 1)
            def _(k=k):
                buf[2, pl.ds(top, half)] = p[k].astype(F32)

            def part(j, i):
                lane = lax.broadcasted_iota(jnp.int32, (32, lanes), 1)
                at = offsets[j] // lanes + i * 32
                r = offsets[j] % lanes
                back = (lanes - r) % lanes
                here = pltpu.roll(buf[j, pl.ds(at, 32)], back, 1)
                then = pltpu.roll(buf[j, pl.ds(at + 1, 32)], back, 1)
                return jnp.where(lane < lanes - r, here, then)

            for low in (True, False):

                @pl.loop(0, half // 32)
                def _(step, k=k, out=out, low=low):
                    i = step if low else step + half // 32
                    lane = lax.broadcasted_iota(jnp.int32, (32, lanes), 1)
                    row = lax.broadcasted_iota(jnp.int32, (32, lanes), 0)
                    position = start + i * (32 * lanes) + row * lanes + lane
                    if low:
                        value = jnp.where(position < first, part(0, i), part(1, i))
                    else:
                        value = jnp.where(position >= end, part(2, i), part(1, i))
                    at = pl.ds(i * 32, 32)
                    out[at] = value
                    state[2 + k, at] = value.astype(BF)

        high = w[...].astype(BF)
        state[0] = high
        state[1] = (w[...] - high.astype(F32)).astype(BF)

    size = rows * lanes
    outs = [pltpu.VMEM((rows, lanes), F32)] * 2 + [pltpu.VMEM((4, rows, lanes), BF)]
    return call(
        body,
        where,
        (m_old, v_old, before, after, passed, master),
        outs,
        [pltpu.VMEM((3, reach, lanes), F32)],
        40 * size,
        40 * size,
    )


def step(grads, master, m_old, v_old, old_bounds):
    count = 128
    width = master.shape[0]
    rows = width // 128
    device = lax.axis_index(DP)
    z, y, x, c = coords(device)
    places = table(z, y, x, c)
    mine = [16 * s for s in range(4)]
    theirs = [64 + 16 * s for s in range(4)]
    g = grads[0].reshape(128, rows, 128)

    given, kept, swapped = {}, {}, {}
    given[2], given[1], given[3] = fetch(places, g, *((theirs[k], BF) for k in (2, 1, 3)))
    for k in (2, 1, 3):
        swapped[k] = send(given[k], "core")
    kept[2], kept[1], kept[3], given[0], kept[0] = fetch(
        places, g, (mine[2], F32), (mine[1], F32), (mine[3], F32), (theirs[0], BF), (mine[0], F32)
    )
    swapped[0] = send(given[0], "core")

    low, high = (0, 8), (8, 8)

    def local_sum(s, half, *more):
        (value,) = sum_piece([[(kept[s], *half)], [(swapped[s], *half)]] + [[(v, 0, 8)] for v in more], [(8, BF)])
        return value

    two_low, two_high = sum_piece([[(kept[2], 0, 16)], [(swapped[2], 0, 16)]], [(8, BF)] * 2)
    passing_low = send(two_low, "a", 1)
    passing_high = send(two_high, "a", 3)
    left_high = send(local_sum(1, high), "a", 1)
    right_low = send(local_sum(3, low), "a", 3)
    joined_low = local_sum(1, low, passing_low)
    left_low = send(joined_low, "a", 1)
    joined_high = local_sum(3, high, passing_high)
    right_high = send(joined_high, "a", 3)
    master_tiles = master.reshape(rows, 128)
    m_tiles, v_tiles = m_old[0].reshape(-1, 128), v_old[0].reshape(-1, 128)
    where = jnp.concatenate([old_bounds, device[None].astype(jnp.int32)])
    up, down = packed_moments(where, m_tiles, v_tiles, rows // 2)
    before = lax.ppermute(up, DP, [(d, d + 1) for d in range(127)])
    after = send(down, "core")
    passed = lax.ppermute(after, DP, [(d, d - 2) for d in range(3, 128, 2)])
    m_prev, v_prev, state = old_moments(where, m_tiles, v_tiles, before, after, passed, master_tiles)
    states = [state] + [None] * 3
    for s in (2, 1, 3):
        states[4 - s] = send(state, "z", s)
    own, q1, q2, q3 = sum_piece(
        [
            [(kept[0], 0, 16)],
            [(swapped[0], 0, 16)],
            [(left_low, 0, 8), (left_high, 0, 8)],
            [(right_low, 0, 8), (right_high, 0, 8)],
        ],
        [(4, F32)] + [(4, BF)] * 3,
    )
    quarters = {2: q2, 1: q1, 3: q3}
    for s in (2, 1, 3):
        quarters[s] = send(quarters[s], "b", s)
    (partial,) = sum_piece([[(v, 0, 4)] for v in (own, quarters[1], quarters[2], quarters[3])], [(4, BF)])
    parts = {}
    for s in (2, 1, 3):
        parts[s] = send(partial, "z", s)
    gradient, squares = total_piece(partial, parts[1], parts[2], parts[3], 32)
    squares = lax.all_to_all(squares, ("y", "x", "core"), 0, 0, tiled=True)
    piece, clip = updated_piece(gradient, states, squares, count * width)
    new = adam(master_tiles, m_prev, v_prev, gradient[0], clip[0, 0])
    master_new, m_new, v_new = (value.reshape(width) for value in new)

    got = {}
    for s in (3, 2, 1):
        got[s] = send(piece, "b", s)
    halves = {}
    halves[0, 0] = joined(piece, got[3])
    halves[0, 1] = joined(got[2], got[1])
    for h in range(2):
        halves[3, h] = send(halves[0, h], "a", 1)
        halves[1, h] = send(halves[0, h], "a", 3)
    halves[2, 0] = send(halves[3, 0], "a", 1)
    halves[2, 1] = send(halves[1, 1], "a", 3)
    partner = {}
    for r, h in halves:
        partner[r, h] = send(halves[r, h], "core")
    out = None
    for keys in (((0, 0), (0, 1)), ((3, 0), (1, 0), (3, 1), (1, 1)), ((2, 0), (2, 1))):
        pairs = [(mine[r] + 8 * h, halves[r, h]) for r, h in keys]
        pairs += [(theirs[r] + 8 * h, partner[r, h]) for r, h in keys]
        out = place(places, pairs, out)
    return (master_new, m_new, v_new, out.reshape(count * width))


def solution(mesh):
    finer = Mesh(mesh.devices.reshape(4, 4, 4, 2), DP)
    placed = (P(DP, None), P(DP), P(DP, None), P(DP, None), P())
    return jax.shard_map(step, mesh=finer, in_specs=placed, out_specs=(P(DP), P(DP), P(DP), P()), check_vma=False)
```

```python
import jax
import jax.numpy as jnp
from jax import lax
from jax.experimental import pallas as pl
from jax.experimental.pallas import tpu as pltpu
from jax.sharding import Mesh
from jax.sharding import PartitionSpec as P

DP = ("z", "y", "x", "core")
BF = jnp.bfloat16
F32 = jnp.float32


def coords(d):
    return d // 32, d // 8 % 4, d // 2 % 4, d % 2


def shard_of(z, y, x, c):
    return ((z * 4 + y) * 4 + x) * 2 + c


def perm(axis, s):
    pairs = []
    for d in range(128):
        z, y, x, c = coords(d)
        if axis == "core":
            c = 1 - c
        elif axis == "z":
            z = (z + s) % 4
        elif (axis == "a") == (c == 0):
            x = (x + s) % 4
        else:
            y = (y + s) % 4
        pairs.append((d, shard_of(z, y, x, c)))
    return pairs


def send(value, axis, s=1):
    return lax.ppermute(value, DP, perm(axis, s))


def table(z, y, x, core):
    i = jnp.arange(128, dtype=jnp.int32)
    c = (core + i // 64) % 2
    s, rb, rz = i // 16 % 4, i // 4 % 4, i % 4
    zz = (z + rz) % 4
    on_0 = shard_of(zz, (y + rb) % 4, (x + s) % 4, 0)
    on_1 = shard_of(zz, (y + s) % 4, (x + rb) % 4, 1)
    return jnp.where(c == 0, on_0, on_1).astype(jnp.int32)


def cost(flops, nbytes):
    return pl.CostEstimate(flops=flops, transcendentals=0, bytes_accessed=nbytes)


def call(body, t, operands, outs, scratch, flops, nbytes, aliases=None, spaces=None, limit=8):
    vmem = pl.BlockSpec(memory_space=pltpu.VMEM)
    hbm = pl.BlockSpec(memory_space=pltpu.HBM)
    spaces = spaces or [True] * len(operands)
    operands = [pltpu.with_memory_space_constraint(o, pltpu.VMEM if v else pltpu.HBM) for o, v in zip(operands, spaces)]
    return pl.pallas_call(
        body,
        grid_spec=pltpu.PrefetchScalarGridSpec(
            num_scalar_prefetch=1,
            grid=(1,),
            in_specs=[vmem if v else hbm for v in spaces],
            out_specs=[hbm if isinstance(o, jax.ShapeDtypeStruct) else vmem for o in outs],
            scratch_shapes=scratch,
        ),
        out_shape=outs,
        input_output_aliases=aliases or {},
        cost_estimate=cost(flops, nbytes),
        compiler_params=pltpu.CompilerParams(vmem_limit_bytes=limit * 2**20),
    )(t, *operands)


def fetch(t, g, *pieces):
    _, rows, lanes = g.shape
    n = 16
    kept = [dtype == g.dtype for _, dtype in pieces]
    m = len(pieces)

    def body(t_ref, g_ref, *refs):
        outs, rest = refs[:m], refs[m:]
        sem, buf = rest[-1], rest[0]
        copies = []
        for k in range(m):
            slot = sum(not v for v in kept[:k]) * n
            for i in range(n):
                to = outs[k].at[i] if kept[k] else buf.at[slot + i]
                copies.append((k, i, slot + i, pltpu.make_async_copy(g_ref.at[t_ref[pieces[k][0] + i]], to, sem.at[k * n + i])))
        for *_, copy in copies:
            copy.start()
        for k, i, at, copy in copies:
            copy.wait()
            if not kept[k]:
                outs[k][i] = buf[at].astype(outs[k].dtype)

    converted = m - sum(kept)
    scratch = [pltpu.VMEM((converted * n, rows, lanes), g.dtype)] if converted else []
    size = m * n * rows * lanes
    return call(
        body,
        t,
        (g,),
        [pltpu.VMEM((n, rows, lanes), dtype) for _, dtype in pieces],
        scratch + [pltpu.SemaphoreType.DMA((m * n,))],
        size,
        6 * size,
        spaces=[False],
        limit=2 + 2 * converted,
    )


def sum_piece(parts, kinds):
    rows, lanes = parts[0][0][0].shape[1:]
    operands = [array for part in parts for array, _, _ in part]

    def sources(base):
        at = 0
        for part in parts:
            begin = 0
            for k, (_, first, count) in enumerate(part):
                if begin <= base < begin + count:
                    yield at + k, first + base - begin
                begin += count
            at += len(part)

    def body(t_ref, *refs):
        ins, outs = refs[: len(operands)], refs[len(operands) :]
        base = 0
        for o, (count, _) in zip(outs, kinds):
            where = list(sources(base))

            @pl.loop(0, count)
            def _(i, o=o, where=where):
                value = None
                for k, first in where:
                    term = ins[k][first + i].astype(F32)
                    value = term if value is None else value + term
                o[i] = value.astype(o.dtype)

            base += count

    size = sum(count for count, _ in kinds) * rows * lanes
    outs = [pltpu.VMEM((count, rows, lanes), dtype) for count, dtype in kinds]
    return call(body, jnp.zeros((1,), jnp.int32), operands, outs, [], len(parts) * size, (4 + 2 * len(parts)) * size)


def joined(first, second):
    def body(t_ref, a, b, o):
        o[: a.shape[0]] = a[...]
        o[a.shape[0] :] = b[...]

    shape = (first.shape[0] + second.shape[0], *first.shape[1:])
    n = first.size + second.size
    outs = [pltpu.VMEM(shape, first.dtype)]
    return call(body, jnp.zeros((1,), jnp.int32), (first, second), outs, [], n, 4 * n)[0]


def place(t, pairs, out):
    k = len(pairs)
    rows, lanes = pairs[0][1].shape[1:]
    counts = [piece.shape[0] for _, piece in pairs]

    def body(t_ref, *refs):
        o, sem = refs[-2:]
        copies = []
        for j, (first, _) in enumerate(pairs):
            for i in range(counts[j]):
                copies.append(pltpu.make_async_copy(refs[j].at[i], o.at[t_ref[first + i]], sem.at[len(copies)]))
        for copy in copies:
            copy.start()
        for copy in copies:
            copy.wait()

    operands = [piece for _, piece in pairs] + ([] if out is None else [out])
    nbytes = 4 * sum(counts) * rows * lanes
    return call(
        body,
        t,
        operands,
        [jax.ShapeDtypeStruct((128, rows, lanes), BF)],
        [pltpu.SemaphoreType.DMA((sum(counts),))],
        nbytes,
        nbytes,
        {} if out is None else {k + 1: 0},
        [True] * k + [False] * (0 if out is None else 1),
    )[0]


def total_piece(own, from1, from2, from3, copies):
    n, rows, lanes = own.shape

    def body(t_ref, w, x1, x2, x3, g, squares):
        sums = []
        for r in range(n):

            def step(i, acc, r=r):
                at = pl.ds(i * 16, 16)
                even = w[r, at].astype(F32) + x2[(r + 2) % n, at].astype(F32)
                odd = x1[(r + 1) % n, at].astype(F32) + x3[(r + 3) % n, at].astype(F32)
                value = even + odd
                g[r, at] = value
                return acc + value * value

            sums.append(lax.fori_loop(0, rows // 16, step, jnp.zeros((16, lanes), F32)))
        acc = (sums[0] + sums[2]) + (sums[1] + sums[3])
        squares[...] = jnp.broadcast_to(jnp.sum(acc), squares.shape)

    size = n * rows * lanes
    outs = [pltpu.VMEM((n, rows, lanes), F32), pltpu.VMEM((copies, 8, lanes), F32)]
    return call(body, jnp.zeros((1,), jnp.int32), (own, from1, from2, from3), outs, [], 6 * size, 12 * size)


def adam(master, m_prev, v_prev, gradient, clip):
    clipped = clip * gradient
    m_new = 0.5 * m_prev + 0.5 * clipped
    v_new = 0.95 * v_prev + 0.05 * clipped * clipped
    direction = m_new / (1.0 - 0.5**20) / (jnp.sqrt(v_new / (1.0 - 0.95**20)) + 1e-08)
    return master - 0.05 * (direction + 0.1 * master), m_new, v_new


def updated_piece(gradient, states, squares, flat):
    n, rows, lanes = gradient.shape

    def body(t_ref, g, *refs):
        state, part, piece, clip_ref = refs[:n], refs[n], refs[n + 1], refs[n + 2]
        total = part[0]
        for i in range(1, part.shape[0]):
            total = total + part[i]
        clip = jnp.minimum(1.0, jnp.sqrt(jnp.float32(flat)) / (jnp.sqrt(total) + 1e-06))
        clip_ref[...] = clip
        clip = jnp.concatenate([clip, clip])
        for r in range(n):

            @pl.loop(0, rows // 16)
            def _(i, r=r):
                at = pl.ds(i * 16, 16)
                high, low, m, v = (state[r][k, at].astype(F32) for k in range(4))
                piece[r, at] = adam(high + low, m, v, g[r, at], clip)[0].astype(BF)

    size = n * rows * lanes
    outs = [pltpu.VMEM((n, rows, lanes), BF), pltpu.VMEM((8, lanes), F32)]
    return call(body, jnp.zeros((1,), jnp.int32), (gradient, *states, squares), outs, [], 20 * size, 14 * size)


def moved_rows(end, half, lanes, total):
    return jnp.minimum(jnp.maximum(end - half * lanes, 0) // lanes, total - half - 8)


def packed_moments(where, m_old, v_old, half):
    total, lanes = m_old.shape
    last = where.shape[0] - 1

    def body(t_ref, m, v, up, down):
        d = t_ref[last]
        q = moved_rows(t_ref[d + 1] - t_ref[d], half, lanes, total)
        for k, old in enumerate((m, v)):
            up[k] = old[pl.ds(q, half + 8)].astype(BF)
            down[k] = old[pl.ds(0, half)].astype(BF)

    n = 4 * half * lanes
    outs = [pltpu.VMEM((2, half + 8, lanes), BF), pltpu.VMEM((2, half, lanes), BF)]
    return call(body, where, (m_old, v_old), outs, [], n, 6 * n)


def old_moments(where, m_old, v_old, before, after, passed, master):
    rows, lanes = master.shape
    total = m_old.shape[0]
    half = rows // 2
    top = 392
    reach = top + total + half + 8
    last = where.shape[0] - 1

    def body(t_ref, m, v, b, a, p, w, m_out, v_out, state, buf):
        d = t_ref[last]
        start = d * (rows * lanes)
        first = t_ref[d]
        end = t_ref[d + 1]
        ahead = t_ref[jnp.maximum(d - 1, 0)]
        q = moved_rows(first - ahead, half, lanes, total)
        offsets = [start - s + top * lanes for s in (ahead + q * lanes, first, end)]
        for k, (old, out) in enumerate(((m, m_out), (v, v_out))):
            buf[0, pl.ds(top, half + 8)] = b[k].astype(F32)
            buf[1, pl.ds(top, total)] = old[...]

            @pl.when(d % 2 == 0)
            def _(k=k):
                buf[2, pl.ds(top, half)] = a[k].astype(F32)

            @pl.when(d % 2 == 1)
            def _(k=k):
                buf[2, pl.ds(top, half)] = p[k].astype(F32)

            def part(j, i):
                lane = lax.broadcasted_iota(jnp.int32, (32, lanes), 1)
                at = offsets[j] // lanes + i * 32
                r = offsets[j] % lanes
                back = (lanes - r) % lanes
                here = pltpu.roll(buf[j, pl.ds(at, 32)], back, 1)
                then = pltpu.roll(buf[j, pl.ds(at + 1, 32)], back, 1)
                return jnp.where(lane < lanes - r, here, then)

            for low in (True, False):

                @pl.loop(0, half // 32)
                def _(step, k=k, out=out, low=low):
                    i = step if low else step + half // 32
                    lane = lax.broadcasted_iota(jnp.int32, (32, lanes), 1)
                    row = lax.broadcasted_iota(jnp.int32, (32, lanes), 0)
                    position = start + i * (32 * lanes) + row * lanes + lane
                    if low:
                        value = jnp.where(position < first, part(0, i), part(1, i))
                    else:
                        value = jnp.where(position >= end, part(2, i), part(1, i))
                    at = pl.ds(i * 32, 32)
                    out[at] = value
                    state[2 + k, at] = value.astype(BF)

        high = w[...].astype(BF)
        state[0] = high
        state[1] = (w[...] - high.astype(F32)).astype(BF)

    size = rows * lanes
    outs = [pltpu.VMEM((rows, lanes), F32)] * 2 + [pltpu.VMEM((4, rows, lanes), BF)]
    return call(
        body,
        where,
        (m_old, v_old, before, after, passed, master),
        outs,
        [pltpu.VMEM((3, reach, lanes), F32)],
        40 * size,
        40 * size,
    )


def step(grads, master, m_old, v_old, old_bounds):
    count = 128
    width = master.shape[0]
    rows = width // 128
    device = lax.axis_index(DP)
    z, y, x, c = coords(device)
    places = table(z, y, x, c)
    mine = [16 * s for s in range(4)]
    theirs = [64 + 16 * s for s in range(4)]
    g = grads[0].reshape(128, rows, 128)

    given, kept, swapped = {}, {}, {}
    given[2], given[1], given[3] = fetch(places, g, *((theirs[k], BF) for k in (2, 1, 3)))
    for k in (2, 1, 3):
        swapped[k] = send(given[k], "core")
    kept[2], kept[1], kept[3], given[0], kept[0] = fetch(
        places, g, (mine[2], F32), (mine[1], F32), (mine[3], F32), (theirs[0], BF), (mine[0], F32)
    )
    swapped[0] = send(given[0], "core")

    low, high = (0, 8), (8, 8)

    def local_sum(s, half, *more):
        (value,) = sum_piece([[(kept[s], *half)], [(swapped[s], *half)]] + [[(v, 0, 8)] for v in more], [(8, BF)])
        return value

    two_low, two_high = sum_piece([[(kept[2], 0, 16)], [(swapped[2], 0, 16)]], [(8, BF)] * 2)
    passing_low = send(two_low, "a", 1)
    passing_high = send(two_high, "a", 3)
    left_high = send(local_sum(1, high), "a", 1)
    right_low = send(local_sum(3, low), "a", 3)
    joined_low = local_sum(1, low, passing_low)
    left_low = send(joined_low, "a", 1)
    joined_high = local_sum(3, high, passing_high)
    right_high = send(joined_high, "a", 3)
    master_tiles = master.reshape(rows, 128)
    m_tiles, v_tiles = m_old[0].reshape(-1, 128), v_old[0].reshape(-1, 128)
    where = jnp.concatenate([old_bounds, device[None].astype(jnp.int32)])
    up, down = packed_moments(where, m_tiles, v_tiles, rows // 2)
    before = lax.ppermute(up, DP, [(d, d + 1) for d in range(127)])
    after = send(down, "core")
    passed = lax.ppermute(after, DP, [(d, d - 2) for d in range(3, 128, 2)])
    m_prev, v_prev, state = old_moments(where, m_tiles, v_tiles, before, after, passed, master_tiles)
    states = [state] + [None] * 3
    for s in (2, 1, 3):
        states[4 - s] = send(state, "z", s)
    own, q1, q2, q3 = sum_piece(
        [
            [(kept[0], 0, 16)],
            [(swapped[0], 0, 16)],
            [(left_low, 0, 8), (left_high, 0, 8)],
            [(right_low, 0, 8), (right_high, 0, 8)],
        ],
        [(4, F32)] + [(4, BF)] * 3,
    )
    quarters = {2: q2, 1: q1, 3: q3}
    for s in (2, 1, 3):
        quarters[s] = send(quarters[s], "b", s)
    (partial,) = sum_piece([[(v, 0, 4)] for v in (own, quarters[1], quarters[2], quarters[3])], [(4, BF)])
    last = {}
    for s in (2, 1, 3):
        last[s] = send(partial, "z", s)
    gradient, squares = total_piece(partial, last[1], last[2], last[3], 32)
    squares = lax.all_to_all(squares, ("y", "x", "core"), 0, 0, tiled=True)
    piece, clip = updated_piece(gradient, states, squares, count * width)
    new = adam(master_tiles, m_prev, v_prev, gradient[0], clip[0, 0])
    master_new, m_new, v_new = (value.reshape(width) for value in new)

    got = {}
    for s in (3, 2, 1):
        got[s] = send(piece, "b", s)
    parts = {}
    parts[0, 0] = joined(piece, got[3])
    parts[0, 1], parts[0, 2] = got[2], got[1]
    for p in range(3):
        parts[1, p] = send(parts[0, p], "a", 3)
        parts[3, p] = send(parts[0, p], "a", 1)
    parts[2, 0] = send(parts[3, 0], "a", 1)
    for p in (1, 2):
        parts[2, p] = send(parts[1, p], "a", 3)
    partner = {}
    for r, p in parts:
        partner[r, p] = send(parts[r, p], "core")
    out = None
    for near in ((0, 3, 1), (2,)):
        keys = [(r, p) for r in near for p in range(3)]
        pairs = [(mine[r] + (0, 8, 12)[p], parts[r, p]) for r, p in keys]
        pairs += [(theirs[r] + (0, 8, 12)[p], partner[r, p]) for r, p in keys]
        out = place(places, pairs, out)
    return (master_new, m_new, v_new, out.reshape(count * width))


def solution(mesh):
    finer = Mesh(mesh.devices.reshape(4, 4, 4, 2), DP)
    placed = (P(DP, None), P(DP), P(DP, None), P(DP, None), P())
    return jax.shard_map(step, mesh=finer, in_specs=placed, out_specs=(P(DP), P(DP), P(DP), P()), check_vma=False)
```

```python
import jax
import jax.numpy as jnp
from jax import lax
from jax.experimental import pallas as pl
from jax.experimental.pallas import tpu as pltpu
from jax.sharding import Mesh
from jax.sharding import PartitionSpec as P

DP = ("z", "y", "x", "core")
BF = jnp.bfloat16
F32 = jnp.float32


def coords(d):
    return d // 32, d // 8 % 4, d // 2 % 4, d % 2


def shard_of(z, y, x, c):
    return ((z * 4 + y) * 4 + x) * 2 + c


def perm(axis, s):
    pairs = []
    for d in range(128):
        z, y, x, c = coords(d)
        if axis == "core":
            c = 1 - c
        elif axis == "z":
            z = (z + s) % 4
        elif (axis == "a") == (c == 0):
            x = (x + s) % 4
        else:
            y = (y + s) % 4
        pairs.append((d, shard_of(z, y, x, c)))
    return pairs


def send(value, axis, s=1):
    return lax.ppermute(value, DP, perm(axis, s))


def table(z, y, x, core):
    i = jnp.arange(128, dtype=jnp.int32)
    c = (core + i // 64) % 2
    s, rb, rz = i // 16 % 4, i // 4 % 4, i % 4
    zz = (z + rz) % 4
    on_0 = shard_of(zz, (y + rb) % 4, (x + s) % 4, 0)
    on_1 = shard_of(zz, (y + s) % 4, (x + rb) % 4, 1)
    return jnp.where(c == 0, on_0, on_1).astype(jnp.int32)


def cost(flops, nbytes):
    return pl.CostEstimate(flops=flops, transcendentals=0, bytes_accessed=nbytes)


def call(body, t, operands, outs, scratch, flops, nbytes, aliases=None, spaces=None, limit=8):
    vmem = pl.BlockSpec(memory_space=pltpu.VMEM)
    hbm = pl.BlockSpec(memory_space=pltpu.HBM)
    spaces = spaces or [True] * len(operands)
    operands = [pltpu.with_memory_space_constraint(o, pltpu.VMEM if v else pltpu.HBM) for o, v in zip(operands, spaces)]
    return pl.pallas_call(
        body,
        grid_spec=pltpu.PrefetchScalarGridSpec(
            num_scalar_prefetch=1,
            grid=(1,),
            in_specs=[vmem if v else hbm for v in spaces],
            out_specs=[hbm if isinstance(o, jax.ShapeDtypeStruct) else vmem for o in outs],
            scratch_shapes=scratch,
        ),
        out_shape=outs,
        input_output_aliases=aliases or {},
        cost_estimate=cost(flops, nbytes),
        compiler_params=pltpu.CompilerParams(vmem_limit_bytes=limit * 2**20),
    )(t, *operands)


def fetch(t, g, *pieces):
    _, rows, lanes = g.shape
    n = 16
    kept = [dtype == g.dtype for _, dtype in pieces]
    m = len(pieces)

    def body(t_ref, g_ref, *refs):
        outs, rest = refs[:m], refs[m:]
        sem, buf = rest[-1], rest[0]
        copies = []
        for k in range(m):
            slot = sum(not v for v in kept[:k]) * n
            for i in range(n):
                to = outs[k].at[i] if kept[k] else buf.at[slot + i]
                copies.append((k, i, slot + i, pltpu.make_async_copy(g_ref.at[t_ref[pieces[k][0] + i]], to, sem.at[k * n + i])))
        for *_, copy in copies:
            copy.start()
        for k, i, at, copy in copies:
            copy.wait()
            if not kept[k]:
                outs[k][i] = buf[at].astype(outs[k].dtype)

    converted = m - sum(kept)
    scratch = [pltpu.VMEM((converted * n, rows, lanes), g.dtype)] if converted else []
    size = m * n * rows * lanes
    return call(
        body,
        t,
        (g,),
        [pltpu.VMEM((n, rows, lanes), dtype) for _, dtype in pieces],
        scratch + [pltpu.SemaphoreType.DMA((m * n,))],
        size,
        6 * size,
        spaces=[False],
        limit=2 + 2 * converted,
    )


def sum_piece(parts, kinds):
    rows, lanes = parts[0][0][0].shape[1:]
    operands = [array for part in parts for array, _, _ in part]

    def sources(base):
        at = 0
        for part in parts:
            begin = 0
            for k, (_, first, count) in enumerate(part):
                if begin <= base < begin + count:
                    yield at + k, first + base - begin
                begin += count
            at += len(part)

    def body(t_ref, *refs):
        ins, outs = refs[: len(operands)], refs[len(operands) :]
        base = 0
        for o, (count, _) in zip(outs, kinds):
            where = list(sources(base))

            @pl.loop(0, count)
            def _(i, o=o, where=where):
                value = None
                for k, first in where:
                    term = ins[k][first + i].astype(F32)
                    value = term if value is None else value + term
                o[i] = value.astype(o.dtype)

            base += count

    size = sum(count for count, _ in kinds) * rows * lanes
    outs = [pltpu.VMEM((count, rows, lanes), dtype) for count, dtype in kinds]
    return call(body, jnp.zeros((1,), jnp.int32), operands, outs, [], len(parts) * size, (4 + 2 * len(parts)) * size)


def joined(first, second):
    def body(t_ref, a, b, o):
        o[: a.shape[0]] = a[...]
        o[a.shape[0] :] = b[...]

    shape = (first.shape[0] + second.shape[0], *first.shape[1:])
    n = first.size + second.size
    outs = [pltpu.VMEM(shape, first.dtype)]
    return call(body, jnp.zeros((1,), jnp.int32), (first, second), outs, [], n, 4 * n)[0]


def place(t, pairs, out):
    k = len(pairs)
    rows, lanes = pairs[0][1].shape[1:]
    counts = [piece.shape[0] for _, piece in pairs]

    def body(t_ref, *refs):
        o, sem = refs[-2:]
        copies = []
        for j, (first, _) in enumerate(pairs):
            for i in range(counts[j]):
                copies.append(pltpu.make_async_copy(refs[j].at[i], o.at[t_ref[first + i]], sem.at[len(copies)]))
        for copy in copies:
            copy.start()
        for copy in copies:
            copy.wait()

    operands = [piece for _, piece in pairs] + ([] if out is None else [out])
    nbytes = 4 * sum(counts) * rows * lanes
    return call(
        body,
        t,
        operands,
        [jax.ShapeDtypeStruct((128, rows, lanes), BF)],
        [pltpu.SemaphoreType.DMA((sum(counts),))],
        nbytes,
        nbytes,
        {} if out is None else {k + 1: 0},
        [True] * k + [False] * (0 if out is None else 1),
    )[0]


def total_piece(own, from1, from2, from3, copies):
    n, rows, lanes = own.shape

    def body(t_ref, w, x1, x2, x3, g, squares):
        sums = []
        for r in range(n):

            def step(i, acc, r=r):
                at = pl.ds(i * 16, 16)
                even = w[r, at].astype(F32) + x2[(r + 2) % n, at].astype(F32)
                odd = x1[(r + 1) % n, at].astype(F32) + x3[(r + 3) % n, at].astype(F32)
                value = even + odd
                g[r, at] = value
                return acc + value * value

            sums.append(lax.fori_loop(0, rows // 16, step, jnp.zeros((16, lanes), F32)))
        acc = (sums[0] + sums[2]) + (sums[1] + sums[3])
        squares[...] = jnp.broadcast_to(jnp.sum(acc), squares.shape)

    size = n * rows * lanes
    outs = [pltpu.VMEM((n, rows, lanes), F32), pltpu.VMEM((copies, 1, lanes), F32)]
    return call(body, jnp.zeros((1,), jnp.int32), (own, from1, from2, from3), outs, [], 6 * size, 12 * size)


def adam(master, m_prev, v_prev, gradient, clip):
    clipped = clip * gradient
    m_new = 0.5 * m_prev + 0.5 * clipped
    v_new = 0.95 * v_prev + 0.05 * clipped * clipped
    direction = m_new / (1.0 - 0.5**20) / (jnp.sqrt(v_new / (1.0 - 0.95**20)) + 1e-08)
    return master - 0.05 * (direction + 0.1 * master), m_new, v_new


def updated_piece(gradient, states, squares, flat):
    n, rows, lanes = gradient.shape

    def body(t_ref, g, *refs):
        state, part, piece, clip_ref = refs[:n], refs[n], refs[n + 1], refs[n + 2]
        total = part[0]
        for i in range(1, part.shape[0]):
            total = total + part[i]
        clip = jnp.minimum(1.0, jnp.sqrt(jnp.float32(flat)) / (jnp.sqrt(total) + 1e-06))
        clip_ref[...] = jnp.broadcast_to(clip, clip_ref.shape)
        clip = jnp.broadcast_to(clip, (16, lanes))
        for r in range(n):

            @pl.loop(0, rows // 16)
            def _(i, r=r):
                at = pl.ds(i * 16, 16)
                high, low, m, v = (state[r][k, at].astype(F32) for k in range(4))
                piece[r, at] = adam(high + low, m, v, g[r, at], clip)[0].astype(BF)

    size = n * rows * lanes
    outs = [pltpu.VMEM((n, rows, lanes), BF), pltpu.VMEM((8, lanes), F32)]
    return call(body, jnp.zeros((1,), jnp.int32), (gradient, *states, squares), outs, [], 20 * size, 14 * size)


def moved_rows(end, half, lanes, total):
    return jnp.minimum(jnp.maximum(end - half * lanes, 0) // lanes, total - half - 8)


def packed_moments(where, m_old, v_old, half):
    total, lanes = m_old.shape
    last = where.shape[0] - 1

    def body(t_ref, m, v, up, down):
        d = t_ref[last]
        q = moved_rows(t_ref[d + 1] - t_ref[d], half, lanes, total)
        for k, old in enumerate((m, v)):
            up[k] = old[pl.ds(q, half + 8)].astype(BF)
            down[k] = old[pl.ds(0, half)].astype(BF)

    n = 4 * half * lanes
    outs = [pltpu.VMEM((2, half + 8, lanes), BF), pltpu.VMEM((2, half, lanes), BF)]
    return call(body, where, (m_old, v_old), outs, [], n, 6 * n)


def old_moments(where, m_old, v_old, before, after, passed, master):
    rows, lanes = master.shape
    total = m_old.shape[0]
    half = rows // 2
    top = 392
    reach = top + total + half + 8
    last = where.shape[0] - 1

    def body(t_ref, m, v, b, a, p, w, m_out, v_out, state, buf):
        d = t_ref[last]
        start = d * (rows * lanes)
        first = t_ref[d]
        end = t_ref[d + 1]
        ahead = t_ref[jnp.maximum(d - 1, 0)]
        q = moved_rows(first - ahead, half, lanes, total)
        offsets = [start - s + top * lanes for s in (ahead + q * lanes, first, end)]
        for k, (old, out) in enumerate(((m, m_out), (v, v_out))):
            buf[0, pl.ds(top, half + 8)] = b[k].astype(F32)
            buf[1, pl.ds(top, total)] = old[...]

            @pl.when(d % 2 == 0)
            def _(k=k):
                buf[2, pl.ds(top, half)] = a[k].astype(F32)

            @pl.when(d % 2 == 1)
            def _(k=k):
                buf[2, pl.ds(top, half)] = p[k].astype(F32)

            def part(j, i):
                lane = lax.broadcasted_iota(jnp.int32, (32, lanes), 1)
                at = offsets[j] // lanes + i * 32
                r = offsets[j] % lanes
                back = (lanes - r) % lanes
                here = pltpu.roll(buf[j, pl.ds(at, 32)], back, 1)
                then = pltpu.roll(buf[j, pl.ds(at + 1, 32)], back, 1)
                return jnp.where(lane < lanes - r, here, then)

            for low in (True, False):

                @pl.loop(0, half // 32)
                def _(step, k=k, out=out, low=low):
                    i = step if low else step + half // 32
                    lane = lax.broadcasted_iota(jnp.int32, (32, lanes), 1)
                    row = lax.broadcasted_iota(jnp.int32, (32, lanes), 0)
                    position = start + i * (32 * lanes) + row * lanes + lane
                    if low:
                        value = jnp.where(position < first, part(0, i), part(1, i))
                    else:
                        value = jnp.where(position >= end, part(2, i), part(1, i))
                    at = pl.ds(i * 32, 32)
                    out[at] = value
                    state[2 + k, at] = value.astype(BF)

        high = w[...].astype(BF)
        state[0] = high
        state[1] = (w[...] - high.astype(F32)).astype(BF)

    size = rows * lanes
    outs = [pltpu.VMEM((rows, lanes), F32)] * 2 + [pltpu.VMEM((4, rows, lanes), BF)]
    return call(
        body,
        where,
        (m_old, v_old, before, after, passed, master),
        outs,
        [pltpu.VMEM((3, reach, lanes), F32)],
        40 * size,
        40 * size,
    )


def step(grads, master, m_old, v_old, old_bounds):
    count = 128
    width = master.shape[0]
    rows = width // 128
    device = lax.axis_index(DP)
    z, y, x, c = coords(device)
    places = table(z, y, x, c)
    mine = [16 * s for s in range(4)]
    theirs = [64 + 16 * s for s in range(4)]
    g = grads[0].reshape(128, rows, 128)

    given, kept, swapped = {}, {}, {}
    (given[2],) = fetch(places, g, (theirs[2], BF))
    swapped[2] = send(given[2], "core")
    kept[2], given[1], given[3] = fetch(places, g, (mine[2], F32), (theirs[1], BF), (theirs[3], BF))
    for k in (1, 3):
        swapped[k] = send(given[k], "core")
    kept[1], kept[3], given[0], kept[0] = fetch(
        places, g, (mine[1], F32), (mine[3], F32), (theirs[0], BF), (mine[0], F32)
    )
    swapped[0] = send(given[0], "core")

    low, high = (0, 8), (8, 8)

    def local_sum(s, half, *more):
        (value,) = sum_piece([[(kept[s], *half)], [(swapped[s], *half)]] + [[(v, 0, 8)] for v in more], [(8, BF)])
        return value

    two_low, two_high = sum_piece([[(kept[2], 0, 16)], [(swapped[2], 0, 16)]], [(8, BF)] * 2)
    passing_low = send(two_low, "a", 1)
    passing_high = send(two_high, "a", 3)
    left_high = send(local_sum(1, high), "a", 1)
    right_low = send(local_sum(3, low), "a", 3)
    joined_low = local_sum(1, low, passing_low)
    left_low = send(joined_low, "a", 1)
    joined_high = local_sum(3, high, passing_high)
    right_high = send(joined_high, "a", 3)
    master_tiles = master.reshape(rows, 128)
    m_tiles, v_tiles = m_old[0].reshape(-1, 128), v_old[0].reshape(-1, 128)
    where = jnp.concatenate([old_bounds, device[None].astype(jnp.int32)])
    up, down = packed_moments(where, m_tiles, v_tiles, rows // 2)
    before = lax.ppermute(up, DP, [(d, d + 1) for d in range(127)])
    after = send(down, "core")
    passed = lax.ppermute(after, DP, [(d, d - 2) for d in range(3, 128, 2)])
    m_prev, v_prev, state = old_moments(where, m_tiles, v_tiles, before, after, passed, master_tiles)
    states = [state] + [None] * 3
    for s in (2, 1, 3):
        states[4 - s] = send(state, "z", s)
    own, q1, q2, q3 = sum_piece(
        [
            [(kept[0], 0, 16)],
            [(swapped[0], 0, 16)],
            [(left_low, 0, 8), (left_high, 0, 8)],
            [(right_low, 0, 8), (right_high, 0, 8)],
        ],
        [(4, F32)] + [(4, BF)] * 3,
    )
    quarters = {2: q2, 1: q1, 3: q3}
    for s in (2, 1, 3):
        quarters[s] = send(quarters[s], "b", s)
    (partial,) = sum_piece([[(v, 0, 4)] for v in (own, quarters[1], quarters[2], quarters[3])], [(4, BF)])
    last = {}
    for s in (2, 1, 3):
        last[s] = send(partial, "z", s)
    gradient, squares = total_piece(partial, last[1], last[2], last[3], 32)
    squares = lax.all_to_all(squares, ("y", "x", "core"), 0, 0, tiled=True)
    piece, clip = updated_piece(gradient, states, squares, count * width)
    new = adam(master_tiles, m_prev, v_prev, gradient[0], clip[0, 0])
    master_new, m_new, v_new = (value.reshape(width) for value in new)

    got = {}
    for s in (3, 2, 1):
        got[s] = send(piece, "b", s)
    parts = {}
    parts[0, 0] = joined(piece, got[3])
    parts[0, 1], parts[0, 2] = got[2], got[1]
    for p in range(3):
        parts[1, p] = send(parts[0, p], "a", 3)
        parts[3, p] = send(parts[0, p], "a", 1)
    parts[2, 0] = send(parts[3, 0], "a", 1)
    for p in (1, 2):
        parts[2, p] = send(parts[1, p], "a", 3)
    partner = {}
    for r, p in parts:
        partner[r, p] = send(parts[r, p], "core")
    out = None
    for near in ((0, 3, 1), (2,)):
        keys = [(r, p) for r in near for p in range(3)]
        pairs = [(mine[r] + (0, 8, 12)[p], parts[r, p]) for r, p in keys]
        pairs += [(theirs[r] + (0, 8, 12)[p], partner[r, p]) for r, p in keys]
        out = place(places, pairs, out)
    return (master_new, m_new, v_new, out.reshape(count * width))


def solution(mesh):
    finer = Mesh(mesh.devices.reshape(4, 4, 4, 2), DP)
    placed = (P(DP, None), P(DP), P(DP, None), P(DP, None), P())
    return jax.shard_map(step, mesh=finer, in_specs=placed, out_specs=(P(DP), P(DP), P(DP), P()), check_vma=False)
```

```python
import jax
import jax.numpy as jnp
from jax import lax
from jax.experimental import pallas as pl
from jax.experimental.pallas import tpu as pltpu
from jax.sharding import Mesh
from jax.sharding import PartitionSpec as P

DP = ("z", "y", "x", "core")
BF = jnp.bfloat16
F32 = jnp.float32


def coords(d):
    return d // 32, d // 8 % 4, d // 2 % 4, d % 2


def shard_of(z, y, x, c):
    return ((z * 4 + y) * 4 + x) * 2 + c


def perm(axis, s):
    pairs = []
    for d in range(128):
        z, y, x, c = coords(d)
        if axis == "core":
            c = 1 - c
        elif axis == "z":
            z = (z + s) % 4
        elif (axis == "a") == (c == 0):
            x = (x + s) % 4
        else:
            y = (y + s) % 4
        pairs.append((d, shard_of(z, y, x, c)))
    return pairs


def send(value, axis, s=1):
    return lax.ppermute(value, DP, perm(axis, s))


def table(z, y, x, core):
    i = jnp.arange(128, dtype=jnp.int32)
    c = (core + i // 64) % 2
    s, rb, rz = i // 16 % 4, i // 4 % 4, i % 4
    zz = (z + rz) % 4
    on_0 = shard_of(zz, (y + rb) % 4, (x + s) % 4, 0)
    on_1 = shard_of(zz, (y + s) % 4, (x + rb) % 4, 1)
    return jnp.where(c == 0, on_0, on_1).astype(jnp.int32)


def cost(flops, nbytes):
    return pl.CostEstimate(flops=flops, transcendentals=0, bytes_accessed=nbytes)


def call(body, t, operands, outs, scratch, flops, nbytes, aliases=None, spaces=None, limit=8):
    vmem = pl.BlockSpec(memory_space=pltpu.VMEM)
    hbm = pl.BlockSpec(memory_space=pltpu.HBM)
    spaces = spaces or [True] * len(operands)
    operands = [pltpu.with_memory_space_constraint(o, pltpu.VMEM if v else pltpu.HBM) for o, v in zip(operands, spaces)]
    return pl.pallas_call(
        body,
        grid_spec=pltpu.PrefetchScalarGridSpec(
            num_scalar_prefetch=1,
            grid=(1,),
            in_specs=[vmem if v else hbm for v in spaces],
            out_specs=[hbm if isinstance(o, jax.ShapeDtypeStruct) else vmem for o in outs],
            scratch_shapes=scratch,
        ),
        out_shape=outs,
        input_output_aliases=aliases or {},
        cost_estimate=cost(flops, nbytes),
        compiler_params=pltpu.CompilerParams(vmem_limit_bytes=limit * 2**20),
    )(t, *operands)


def fetch(t, g, *pieces):
    _, rows, lanes = g.shape
    n = 16
    kept = [dtype == g.dtype for _, dtype in pieces]
    m = len(pieces)

    def body(t_ref, g_ref, *refs):
        outs, rest = refs[:m], refs[m:]
        sem, buf = rest[-1], rest[0]
        copies = []
        for k in range(m):
            slot = sum(not v for v in kept[:k]) * n
            for i in range(n):
                to = outs[k].at[i] if kept[k] else buf.at[slot + i]
                copies.append((k, i, slot + i, pltpu.make_async_copy(g_ref.at[t_ref[pieces[k][0] + i]], to, sem.at[k * n + i])))
        for *_, copy in copies:
            copy.start()
        for k, i, at, copy in copies:
            copy.wait()
            if not kept[k]:
                outs[k][i] = buf[at].astype(outs[k].dtype)

    converted = m - sum(kept)
    scratch = [pltpu.VMEM((converted * n, rows, lanes), g.dtype)] if converted else []
    size = m * n * rows * lanes
    return call(
        body,
        t,
        (g,),
        [pltpu.VMEM((n, rows, lanes), dtype) for _, dtype in pieces],
        scratch + [pltpu.SemaphoreType.DMA((m * n,))],
        size,
        6 * size,
        spaces=[False],
        limit=2 + 2 * converted,
    )


def sum_piece(parts, kinds):
    rows, lanes = parts[0][0][0].shape[1:]
    operands = [array for part in parts for array, _, _ in part]

    def sources(base):
        at = 0
        for part in parts:
            begin = 0
            for k, (_, first, count) in enumerate(part):
                if begin <= base < begin + count:
                    yield at + k, first + base - begin
                begin += count
            at += len(part)

    def body(t_ref, *refs):
        ins, outs = refs[: len(operands)], refs[len(operands) :]
        base = 0
        for o, (count, _) in zip(outs, kinds):
            where = list(sources(base))

            @pl.loop(0, count)
            def _(i, o=o, where=where):
                value = None
                for k, first in where:
                    term = ins[k][first + i].astype(F32)
                    value = term if value is None else value + term
                o[i] = value.astype(o.dtype)

            base += count

    size = sum(count for count, _ in kinds) * rows * lanes
    outs = [pltpu.VMEM((count, rows, lanes), dtype) for count, dtype in kinds]
    return call(body, jnp.zeros((1,), jnp.int32), operands, outs, [], len(parts) * size, (4 + 2 * len(parts)) * size)


def joined(first, second):
    def body(t_ref, a, b, o):
        o[: a.shape[0]] = a[...]
        o[a.shape[0] :] = b[...]

    shape = (first.shape[0] + second.shape[0], *first.shape[1:])
    n = first.size + second.size
    outs = [pltpu.VMEM(shape, first.dtype)]
    return call(body, jnp.zeros((1,), jnp.int32), (first, second), outs, [], n, 4 * n)[0]


def place(t, pairs, out):
    k = len(pairs)
    rows, lanes = pairs[0][1].shape[1:]
    counts = [piece.shape[0] for _, piece in pairs]

    def body(t_ref, *refs):
        o, sem = refs[-2:]
        copies = []
        for j, (first, _) in enumerate(pairs):
            for i in range(counts[j]):
                copies.append(pltpu.make_async_copy(refs[j].at[i], o.at[t_ref[first + i]], sem.at[len(copies)]))
        for copy in copies:
            copy.start()
        for copy in copies:
            copy.wait()

    operands = [piece for _, piece in pairs] + ([] if out is None else [out])
    nbytes = 4 * sum(counts) * rows * lanes
    return call(
        body,
        t,
        operands,
        [jax.ShapeDtypeStruct((128, rows, lanes), BF)],
        [pltpu.SemaphoreType.DMA((sum(counts),))],
        nbytes,
        nbytes,
        {} if out is None else {k + 1: 0},
        [True] * k + [False] * (0 if out is None else 1),
    )[0]


def total_piece(own, from1, from2, from3, copies):
    n, rows, lanes = own.shape

    def body(t_ref, w, x1, x2, x3, g, squares):
        sums = []
        for r in range(n):

            def step(i, acc, r=r):
                at = pl.ds(i * 16, 16)
                even = w[r, at].astype(F32) + x2[(r + 2) % n, at].astype(F32)
                odd = x1[(r + 1) % n, at].astype(F32) + x3[(r + 3) % n, at].astype(F32)
                value = even + odd
                g[r, at] = value
                return acc + value * value

            sums.append(lax.fori_loop(0, rows // 16, step, jnp.zeros((16, lanes), F32)))
        acc = (sums[0] + sums[2]) + (sums[1] + sums[3])
        squares[...] = jnp.broadcast_to(jnp.sum(acc), squares.shape)

    size = n * rows * lanes
    outs = [pltpu.VMEM((n, rows, lanes), F32), pltpu.VMEM((copies, 1, lanes), F32)]
    return call(body, jnp.zeros((1,), jnp.int32), (own, from1, from2, from3), outs, [], 6 * size, 12 * size)


def adam(master, m_prev, v_prev, gradient, clip):
    clipped = clip * gradient
    m_new = 0.5 * m_prev + 0.5 * clipped
    v_new = 0.95 * v_prev + 0.05 * clipped * clipped
    direction = m_new / (1.0 - 0.5**20) / (jnp.sqrt(v_new / (1.0 - 0.95**20)) + 1e-08)
    return master - 0.05 * (direction + 0.1 * master), m_new, v_new


def updated_piece(gradient, states, squares, flat):
    n, rows, lanes = gradient.shape

    def body(t_ref, g, *refs):
        state, part, piece, clip_ref = refs[:n], refs[n], refs[n + 1], refs[n + 2]
        total = part[0]
        for i in range(1, part.shape[0]):
            total = total + part[i]
        clip = jnp.minimum(1.0, jnp.sqrt(jnp.float32(flat)) / (jnp.sqrt(total) + 1e-06))
        clip_ref[...] = jnp.broadcast_to(clip, clip_ref.shape)
        clip = jnp.broadcast_to(clip, (16, lanes))
        for r in range(n):

            @pl.loop(0, rows // 16)
            def _(i, r=r):
                at = pl.ds(i * 16, 16)
                high, low, m, v = (state[r][k, at].astype(F32) for k in range(4))
                piece[r, at] = adam(high + low, m, v, g[r, at], clip)[0].astype(BF)

    size = n * rows * lanes
    outs = [pltpu.VMEM((n, rows, lanes), BF), pltpu.VMEM((8, lanes), F32)]
    return call(body, jnp.zeros((1,), jnp.int32), (gradient, *states, squares), outs, [], 20 * size, 14 * size)


def moved_rows(end, half, lanes, total):
    return jnp.minimum(jnp.maximum(end - half * lanes, 0) // lanes, total - half - 8)


def packed_moments(where, m_old, v_old, half):
    total, lanes = m_old.shape
    last = where.shape[0] - 1

    def body(t_ref, m, v, up, down):
        d = t_ref[last]
        q = moved_rows(t_ref[d + 1] - t_ref[d], half, lanes, total)
        for k, old in enumerate((m, v)):
            up[k] = old[pl.ds(q, half + 8)].astype(BF)
            down[k] = old[pl.ds(0, half)].astype(BF)

    n = 4 * half * lanes
    outs = [pltpu.VMEM((2, half + 8, lanes), BF), pltpu.VMEM((2, half, lanes), BF)]
    return call(body, where, (m_old, v_old), outs, [], n, 6 * n)


def old_moments(where, m_old, v_old, before, after, passed, master):
    rows, lanes = master.shape
    total = m_old.shape[0]
    half = rows // 2
    top = 392
    reach = top + total + half + 8
    last = where.shape[0] - 1

    def body(t_ref, m, v, b, a, p, w, m_out, v_out, state, buf):
        d = t_ref[last]
        start = d * (rows * lanes)
        first = t_ref[d]
        end = t_ref[d + 1]
        ahead = t_ref[jnp.maximum(d - 1, 0)]
        q = moved_rows(first - ahead, half, lanes, total)
        offsets = [start - s + top * lanes for s in (ahead + q * lanes, first, end)]
        for k, (old, out) in enumerate(((m, m_out), (v, v_out))):
            buf[0, pl.ds(top, half + 8)] = b[k].astype(F32)
            buf[1, pl.ds(top, total)] = old[...]

            @pl.when(d % 2 == 0)
            def _(k=k):
                buf[2, pl.ds(top, half)] = a[k].astype(F32)

            @pl.when(d % 2 == 1)
            def _(k=k):
                buf[2, pl.ds(top, half)] = p[k].astype(F32)

            def part(j, i):
                lane = lax.broadcasted_iota(jnp.int32, (32, lanes), 1)
                at = offsets[j] // lanes + i * 32
                r = offsets[j] % lanes
                back = (lanes - r) % lanes
                here = pltpu.roll(buf[j, pl.ds(at, 32)], back, 1)
                then = pltpu.roll(buf[j, pl.ds(at + 1, 32)], back, 1)
                return jnp.where(lane < lanes - r, here, then)

            for low in (True, False):

                @pl.loop(0, half // 32)
                def _(step, k=k, out=out, low=low):
                    i = step if low else step + half // 32
                    lane = lax.broadcasted_iota(jnp.int32, (32, lanes), 1)
                    row = lax.broadcasted_iota(jnp.int32, (32, lanes), 0)
                    position = start + i * (32 * lanes) + row * lanes + lane
                    if low:
                        value = jnp.where(position < first, part(0, i), part(1, i))
                    else:
                        value = jnp.where(position >= end, part(2, i), part(1, i))
                    at = pl.ds(i * 32, 32)
                    out[at] = value
                    state[2 + k, at] = value.astype(BF)

        high = w[...].astype(BF)
        state[0] = high
        state[1] = (w[...] - high.astype(F32)).astype(BF)

    size = rows * lanes
    outs = [pltpu.VMEM((rows, lanes), F32)] * 2 + [pltpu.VMEM((4, rows, lanes), BF)]
    return call(
        body,
        where,
        (m_old, v_old, before, after, passed, master),
        outs,
        [pltpu.VMEM((3, reach, lanes), F32)],
        40 * size,
        40 * size,
    )


def step(grads, master, m_old, v_old, old_bounds):
    count = 128
    width = master.shape[0]
    rows = width // 128
    device = lax.axis_index(DP)
    z, y, x, c = coords(device)
    places = table(z, y, x, c)
    mine = [16 * s for s in range(4)]
    theirs = [64 + 16 * s for s in range(4)]
    g = grads[0].reshape(128, rows, 128)

    given, kept, swapped = {}, {}, {}
    given[2], given[1], given[3] = fetch(places, g, *((theirs[k], BF) for k in (2, 1, 3)))
    for k in (2, 1, 3):
        swapped[k] = send(given[k], "core")
    kept[2], kept[1], kept[3], given[0], kept[0] = fetch(
        places, g, (mine[2], F32), (mine[1], F32), (mine[3], F32), (theirs[0], BF), (mine[0], F32)
    )
    swapped[0] = send(given[0], "core")

    low, high = (0, 8), (8, 8)

    def local_sum(s, half, *more):
        (value,) = sum_piece([[(kept[s], *half)], [(swapped[s], *half)]] + [[(v, 0, 8)] for v in more], [(8, BF)])
        return value

    two_low, two_high = sum_piece([[(kept[2], 0, 16)], [(swapped[2], 0, 16)]], [(8, BF)] * 2)
    passing_low = send(two_low, "a", 1)
    passing_high = send(two_high, "a", 3)
    left_high = send(local_sum(1, high), "a", 1)
    right_low = send(local_sum(3, low), "a", 3)
    joined_low = local_sum(1, low, passing_low)
    left_low = send(joined_low, "a", 1)
    joined_high = local_sum(3, high, passing_high)
    right_high = send(joined_high, "a", 3)
    master_tiles = master.reshape(rows, 128)
    m_tiles, v_tiles = m_old[0].reshape(-1, 128), v_old[0].reshape(-1, 128)
    where = jnp.concatenate([old_bounds, device[None].astype(jnp.int32)])
    up, down = packed_moments(where, m_tiles, v_tiles, rows // 2)
    before = lax.ppermute(up, DP, [(d, d + 1) for d in range(127)])
    after = send(down, "core")
    passed = lax.ppermute(after, DP, [(d, d - 2) for d in range(3, 128, 2)])
    m_prev, v_prev, state = old_moments(where, m_tiles, v_tiles, before, after, passed, master_tiles)
    states = [state] + [None] * 3
    for s in (2, 1, 3):
        states[4 - s] = send(state, "z", s)
    own, q1, q2, q3 = sum_piece(
        [
            [(kept[0], 0, 16)],
            [(swapped[0], 0, 16)],
            [(left_low, 0, 8), (left_high, 0, 8)],
            [(right_low, 0, 8), (right_high, 0, 8)],
        ],
        [(4, F32)] + [(4, BF)] * 3,
    )
    quarters = {2: q2, 1: q1, 3: q3}
    for s in (2, 1, 3):
        quarters[s] = send(quarters[s], "b", s)
    (partial,) = sum_piece([[(v, 0, 4)] for v in (own, quarters[1], quarters[2], quarters[3])], [(4, BF)])
    parts = {}
    for s in (2, 1, 3):
        parts[s] = send(partial, "z", s)
    gradient, squares = total_piece(partial, parts[1], parts[2], parts[3], 32)
    squares = lax.all_to_all(squares, ("y", "x", "core"), 0, 0, tiled=True)
    piece, clip = updated_piece(gradient, states, squares, count * width)
    new = adam(master_tiles, m_prev, v_prev, gradient[0], clip[0, 0])
    master_new, m_new, v_new = (value.reshape(width) for value in new)

    got = {}
    for s in (3, 2, 1):
        got[s] = send(piece, "b", s)
    halves = {}
    halves[0, 0] = joined(piece, got[3])
    halves[0, 1] = joined(got[2], got[1])
    for h in range(2):
        halves[3, h] = send(halves[0, h], "a", 1)
        halves[1, h] = send(halves[0, h], "a", 3)
    halves[2, 0] = send(halves[3, 0], "a", 1)
    halves[2, 1] = send(halves[1, 1], "a", 3)
    partner = {}
    for r, h in halves:
        partner[r, h] = send(halves[r, h], "core")
    out = None
    for keys in (((0, 0), (0, 1)), ((3, 0), (1, 0), (3, 1), (1, 1)), ((2, 0), (2, 1))):
        pairs = [(mine[r] + 8 * h, halves[r, h]) for r, h in keys]
        pairs += [(theirs[r] + 8 * h, partner[r, h]) for r, h in keys]
        out = place(places, pairs, out)
    return (master_new, m_new, v_new, out.reshape(count * width))


def solution(mesh):
    finer = Mesh(mesh.devices.reshape(4, 4, 4, 2), DP)
    placed = (P(DP, None), P(DP), P(DP, None), P(DP, None), P())
    return jax.shard_map(step, mesh=finer, in_specs=placed, out_specs=(P(DP), P(DP), P(DP), P()), check_vma=False)
```
